32 devices in a mesh: ta: 4 (over x, core), ha: 4 (over z), wa: 2 (over y).
Axes of the slice: x: 2, y: 2, z: 4, core: 2. Of those that a mesh axis runs over, the one named last changes fastest.
Arguments:
- tokens: bfloat16 [1, 16, 32, 16, 1024], P(None, 'ta', 'ha', 'wa'), may hold values from -40 to 40
- norm_gain: float32 [4, 1024], replicated, may hold values from 0.25 to 1.75
- qkv_weight: bfloat16 [3, 1024, 3, 1024], P(None, None, None, 'ta'), may hold values from -0.1875 to 0.1875
- qk_gain: float32 [3, 2, 64], replicated, may hold values from 0.25 to 1.75
- out_weight: bfloat16 [3, 1024, 1024], P(None, 'ta'), may hold values from -0.1875 to 0.1875
- ffn_in: bfloat16 [1024, 2, 2048], P(None, None, 'ta'), may hold values from -0.1875 to 0.1875
- ffn_out: bfloat16 [2048, 1024], P('ta'), may hold values from -0.125 to 0.125
Outputs:
- layer_out: bfloat16 [1, 16, 32, 16, 1024], P(None, 'ta', 'ha', 'wa')
The draws below stay inside these ranges and needn't reach their ends.
All inputs are finite; a program needn't handle non-finite values.
Results may differ from the reference program's by a relative error of at most 0.015.
Values may be sent and summed in bfloat16 or wider, within the bound.
A program may use at most 192 MiB of HBM per device.

```python
import math
import jax
import jax.numpy as jnp
from jax import lax

D = 1024
HEAD_DIM = 64
FF = 2048
CLIPS = 1
ATTN_WIDTH = 1024
FRAMES = 16
HEIGHT = 32
WIDTH = 16
N_TA = 4


def draw_tokens(key, part):
    key_entries, key_column, key_row = jax.random.split(key, 3)
    extent = (CLIPS, FRAMES, HEIGHT, WIDTH, D)
    entries = jnp.clip(jax.random.normal(key_entries, extent, jnp.float32), -4.0, 4.0)
    column_scale = jnp.exp(jax.random.uniform(key_column, (D,), jnp.float32, math.log(0.3), math.log(3.0)))
    row_scale = jnp.exp(jax.random.uniform(key_row, extent[:4] + (1,), jnp.float32, math.log(0.5), math.log(2.0)))
    return (entries * column_scale * row_scale).astype(jnp.bfloat16)


def levels(key, shape, cuts, least, high):
    loudness, own = 1.0, jax.random.fold_in(key, 6)
    for axis_at, blocks in cuts:
        heights = jnp.exp(jax.random.uniform(jax.random.fold_in(own, axis_at), (blocks,), jnp.float32, least / len(cuts), high / len(cuts)))
        loudness = loudness * jnp.repeat(heights, shape[axis_at] // blocks).reshape([-1 if axis == axis_at else 1 for axis in range(len(shape))])
    return loudness


def gaussian(key, shape, spread, bound, shards=(), dtype=jnp.bfloat16):
    result = spread * jax.random.normal(key, shape, jnp.float32)
    if shards:
        result = result * levels(key, shape, shards, -0.22, 0.18)
    return jnp.clip(result, -bound, bound).astype(dtype)


def setup_inputs(seed: int = 0) -> dict:
    streams_of = jax.random.split(jax.random.key(seed), 8)
    return {
        "tokens": draw_tokens(jax.random.fold_in(streams_of[7], 71), 0),
        "norm_gain": jnp.clip(1.0 + 0.15 * jax.random.normal(streams_of[1], (4, D), jnp.float32), 0.25, 1.75),
        "qkv_weight": gaussian(streams_of[2], (3, D, 3, ATTN_WIDTH), D ** -0.5, 0.1875, ((3, 4),)),
        "qk_gain": jnp.clip(1.0 + 0.15 * jax.random.normal(streams_of[3], (3, 2, HEAD_DIM), jnp.float32), 0.25, 1.75),
        "out_weight": gaussian(streams_of[4], (3, ATTN_WIDTH, D), ATTN_WIDTH ** -0.5, 0.1875, ((1, 4),)),
        "ffn_in": gaussian(streams_of[5], (D, 2, FF), D ** -0.5, 0.1875, ((2, 4),)),
        "ffn_out": gaussian(streams_of[6], (FF, D), FF ** -0.5, 0.125, ((0, 4),)),
    }


def rms_norm(stream, gain_row):
    return stream * lax.rsqrt(lax.optimization_barrier(jnp.mean(stream * stream, axis=-1, keepdims=True)) + 1e-06) * gain_row

def head_norm(vectors, gain_row):
    return vectors * lax.rsqrt(lax.optimization_barrier(jnp.mean(vectors * vectors, axis=-1, keepdims=True)) + 1e-06) * gain_row

def grouped_product(left, right):
    inner = left.shape[-1]
    block = inner // N_TA
    left_blocks = left.reshape(-1, N_TA, block).astype(jnp.float32)
    right_blocks = right.reshape(N_TA, block, -1).astype(jnp.float32)
    parts = jnp.einsum('rgk,gkd->grd', left_blocks, right_blocks)
    rounded = lax.optimization_barrier(parts.astype(jnp.bfloat16))
    return lax.optimization_barrier(jnp.sum(rounded.astype(jnp.float32), axis=0))

def project(normed, weight_block, gain_pair):
    extent = normed.shape
    model_width = extent[-1]
    flat_qkv = jnp.dot(normed.reshape(-1, model_width), weight_block.reshape(model_width, -1), preferred_element_type=jnp.float32)
    head_count = weight_block.shape[-1] // HEAD_DIM
    flat_qkv = flat_qkv.reshape(extent[:4] + (3, head_count, HEAD_DIM))
    queries = head_norm(flat_qkv[..., 0, :, :], gain_pair[0])
    key_rows = head_norm(flat_qkv[..., 1, :, :], gain_pair[1])
    stacked = jnp.stack([queries, key_rows, flat_qkv[..., 2, :, :]], axis=4).astype(jnp.bfloat16)
    return stacked.reshape(extent[:4] + (3, head_count * HEAD_DIM))

def attend(packed, line_axis, causal):
    extent = packed.shape
    head_count = extent[-1] // HEAD_DIM
    split_shape = extent[:4] + (head_count, HEAD_DIM)
    queries = packed[..., 0, :].reshape(split_shape).astype(jnp.float32)
    key_rows = packed[..., 1, :].reshape(split_shape).astype(jnp.float32)
    values = packed[..., 2, :].reshape(split_shape).astype(jnp.float32)
    letters = 'cfyx'
    axis_letter = letters[line_axis]
    query_spec = letters.replace(axis_letter, 'q') + 'hd'
    key_spec = letters.replace(axis_letter, 'k') + 'hd'
    score_spec = letters.replace(axis_letter, '') + 'hqk'
    scores = jnp.einsum(query_spec + ',' + key_spec + '->' + score_spec, queries, key_rows) / math.sqrt(HEAD_DIM)
    exponentials = jnp.exp(scores)
    if causal:
        places = jnp.arange(extent[line_axis])
        exponentials = jnp.where(places[:, None] >= places[None, :], exponentials, jnp.zeros_like(exponentials))
    attn_probs = (exponentials / lax.optimization_barrier(jnp.sum(exponentials, axis=-1, keepdims=True))).astype(jnp.bfloat16)
    attended = jnp.einsum(score_spec + ',' + key_spec + '->' + query_spec, attn_probs.astype(jnp.float32), values)
    return attended.reshape(extent[:4] + (extent[-1],)).astype(jnp.bfloat16)

def attention_pass(stream, gain_row, weight_block, gain_pair, out_block, line_axis, causal):
    map_dim = 2 if line_axis == 1 else 1
    normed = rms_norm(stream, gain_row).astype(jnp.bfloat16)
    blocks = jnp.moveaxis(normed, map_dim, 0)

    def one_block(tile_block):
        restored = jnp.expand_dims(tile_block, map_dim)
        packed = project(restored, weight_block, gain_pair)
        attended = attend(packed, line_axis, causal)
        all_width = attended.shape[-1]
        delta_part = grouped_product(attended.reshape(-1, all_width), out_block)
        return jnp.squeeze(delta_part.reshape(restored.shape[:4] + (out_block.shape[1],)), map_dim)
    deltas = lax.map(one_block, blocks)
    return stream + jnp.moveaxis(deltas, 0, map_dim)

def mlp_block(stream, gain_row, ffn_in, ffn_out):
    normed = rms_norm(stream, gain_row).astype(jnp.bfloat16)
    blocks = jnp.moveaxis(normed, 1, 0)
    model_width = ffn_in.shape[0]
    hidden_width = ffn_in.shape[2]

    def one_frame(frame_tokens):
        flat_tokens = frame_tokens.reshape(-1, model_width)
        both_parts = jnp.dot(flat_tokens, ffn_in.reshape(model_width, -1), preferred_element_type=jnp.float32).reshape(-1, 2, hidden_width)
        hidden = (jax.nn.silu(both_parts[:, 0]) * both_parts[:, 1]).astype(jnp.bfloat16)
        return grouped_product(hidden, ffn_out).reshape(frame_tokens.shape)
    deltas = lax.map(one_frame, blocks)
    return stream + jnp.moveaxis(deltas, 0, 1)

def reference(tokens, norm_gain, qkv_weight, qk_gain, out_weight, ffn_in, ffn_out):
    stream = tokens.astype(jnp.float32)
    for pass_index, line_axis in ((0, 3), (1, 2), (2, 1)):
        stream = attention_pass(stream, norm_gain[pass_index], qkv_weight[pass_index], qk_gain[pass_index], out_weight[pass_index], line_axis, line_axis == 1)
    stream = mlp_block(stream, norm_gain[3], ffn_in, ffn_out)
    return stream.astype(jnp.bfloat16)
```

```python
import functools

import jax
import jax.numpy as jnp
from jax import lax
from jax.experimental import pallas as pl
from jax.experimental.pallas import tpu as pltpu
from jax.sharding import PartitionSpec as P

HEAD_DIM = 64
CHUNKS = 2
EPS = 1e-06
MESH = pl.DeviceIdType.MESH
F32 = jnp.float32
BF16 = jnp.bfloat16


def dot(a, b):
    return jnp.dot(a, b, preferred_element_type=F32)


def dot_t(a, b):
    return lax.dot_general(a, b, (((1,), (1,)), ((), ())), preferred_element_type=F32)


def attend(queries, key_rows, values, mask):
    width = queries.shape[-1]
    lane_head = lax.broadcasted_iota(jnp.int32, (1, width), 1) // HEAD_DIM
    total = None
    for head in range(width // HEAD_DIM):
        pick = (lane_head == head).astype(F32).astype(BF16)
        scores = dot_t(queries * pick, key_rows)
        weights = jnp.where(mask, jnp.exp(scores), 0.0)
        probs = weights * (1.0 / jnp.sum(weights, axis=-1, keepdims=True))
        part = dot(probs.astype(BF16), values * pick)
        total = part if total is None else total + part
    return total.astype(BF16)


class Plan:
    def __init__(self, n, n_ta, frames, rows):
        self.n = n
        self.m = frames
        self.unit = rows // frames
        self.low = min(n, frames)
        self.q = frames // self.low
        self.blocks = n_ta * frames // max(n, frames)
        self.u = self.blocks * self.q


def general_kernel(cfg, tok, gain, qkg, wq_h, wo_h, wi_h, wf_h, out, *s):
    n_ta, frames, height, width, plans = cfg
    (stream, gath, wq, wo, wi, wf, pk, a0, a1, res0, res1, att, pk2, att2, pbuf, prec, comb, xrec,
     wsem, ag_s, ag_r, s10, r10, s20, r20, s11, r11, s21, r21, rs_s, rs_r) = s
    rows = tok.shape[0]
    per_frame = height * width
    aw = wo.shape[1]
    me = lax.axis_index("ta")
    core, chip = lax.rem(me, 2), lax.div(me, 2)

    def block_at(k):
        return lax.rem(chip + lax.div(k, 2), 2) * 2 + lax.rem(core + lax.rem(k, 2), 2)

    piece = rows // CHUNKS
    wide = lambda c: pl.ds(pl.multiple_of(c * piece, piece), piece)
    steps = n_ta * CHUNKS
    early = 2 * CHUNKS

    def arrival(i):
        late = i - early
        k = jnp.where(i < early, lax.div(i, CHUNKS), 2 + lax.rem(late, 2))
        c = jnp.where(i < early, lax.rem(i, CHUNKS), lax.div(late, 2))
        return k, c

    def departure(i):
        rest = i - early
        k = jnp.where(i < early, 3 - lax.rem(i, 2), 1 - lax.div(rest, CHUNKS))
        c = jnp.where(i < early, lax.div(i, 2), lax.rem(rest, CHUNKS))
        return k, c

    partner = block_at(1)
    remote = block_at(2)
    pair_last = block_at(3)

    copies = []
    for at in range(3):
        copies.append([
            pltpu.make_async_copy(wq_h.at[at, j], wq.at[at, :, j * aw:(j + 1) * aw], wsem.at[at, j])
            for j in range(3)])
        copies.append([pltpu.make_async_copy(wo_h.at[at], wo.at[at], wsem.at[at, 3])])
    copies.append([pltpu.make_async_copy(wi_h, wi, wsem.at[3, 0])])
    copies.append([pltpu.make_async_copy(wf_h, wf, wsem.at[3, 1])])
    for group in copies:
        for copy in group:
            copy.start()

    def ready(at):
        for copy in copies[at]:
            copy.wait()

    barrier = pltpu.get_barrier_semaphore()
    greets = 0
    for other in (partner, remote):
        pl.semaphore_signal(barrier, inc=1, device_id={"ta": other}, device_id_type=MESH)
        greets += 1
    for axis, plan in plans:
        here = lax.axis_index(axis)
        for step in range(1, plan.n):
            other = lax.rem(here + step, plan.n)
            pl.semaphore_signal(barrier, inc=1, device_id={axis: other}, device_id_type=MESH)
            greets += 1

    def remote_copy(src, dst, send, recv, axis, other):
        return pltpu.make_async_remote_copy(
            src_ref=src, dst_ref=dst, send_sem=send, recv_sem=recv,
            device_id={axis: other}, device_id_type=MESH)

    def norm_own(p, c):
        x = stream[wide(c), :]
        scale = lax.rsqrt(jnp.mean(x * x, axis=-1, keepdims=True) + EPS)
        gath[p, me, wide(c)] = (x * scale * gain[p:p + 1, :]).astype(BF16)

    def ag_copy(p, slot, c):
        block = me if slot < 2 else remote
        other = remote if slot == 1 else partner
        ref = gath.at[p, block, wide(c)]
        return remote_copy(ref, ref, ag_s.at[p, slot, c], ag_r.at[p, slot, c], "ta", other)

    def ag_start(p, c):
        ag_copy(p, 1, c).start()
        ag_copy(p, 0, c).start()

    def ag_wait(p, k, c):
        @pl.when(k == 1)
        def _():
            ag_copy(p, 0, c).wait_recv()

        @pl.when(k == 2)
        def _():
            ag_copy(p, 1, c).wait_recv()
            ag_copy(p, 2, c).start()

        @pl.when(k == 3)
        def _():
            ag_copy(p, 2, c).wait_recv()

    lane_a = lax.broadcasted_iota(jnp.int32, (aw, aw), 0) // HEAD_DIM
    lane_b = lax.broadcasted_iota(jnp.int32, (aw, aw), 1) // HEAD_DIM
    ones = (lane_a == lane_b).astype(F32).astype(BF16)

    def head_norm(x, row):
        square = x * x
        high = square.astype(BF16)
        low = (square - high.astype(F32)).astype(BF16)
        mean = (dot(high, ones) + dot(low, ones)) * (1.0 / HEAD_DIM)
        return x * lax.rsqrt(mean + EPS) * qkg[row:row + 1, :]

    def project(p, b, c):
        flat = dot(gath[p, b, wide(c)], wq[p])
        queries = (head_norm(flat[:, :aw], 2 * p) * (HEAD_DIM ** -0.5)).astype(BF16)
        key_rows = head_norm(flat[:, aw:2 * aw], 2 * p + 1).astype(BF16)
        return queries, key_rows, flat[:, 2 * aw:].astype(BF16)

    def rs_copy(p, slot, c):
        send, recv = rs_s.at[p, slot, c], rs_r.at[p, slot, c]
        if slot == 2:
            return remote_copy(comb.at[p, wide(c)], xrec.at[p, wide(c)], send, recv, "ta", remote)
        return remote_copy(pbuf.at[p, 2 * slot + 1, wide(c)], prec.at[p, slot, wide(c)], send, recv, "ta", partner)

    def rs_put(p, k, c, part):
        pbuf[p, k, wide(c)] = part.astype(BF16)

        @pl.when(k == 1)
        def _():
            rs_copy(p, 0, c).start()

        @pl.when(k == 3)
        def _():
            rs_copy(p, 1, c).start()

    def rs_combine(p, c):
        rs_copy(p, 1, c).wait_recv()
        comb[p, wide(c)] = (pbuf[p, 2, wide(c)].astype(F32) + prec[p, 1, wide(c)].astype(F32)).astype(BF16)
        rs_copy(p, 2, c).start()

    def rs_total(p, c):
        rs_copy(p, 0, c).wait_recv()
        near = pbuf[p, 0, wide(c)].astype(F32) + prec[p, 0, wide(c)].astype(F32)
        rs_copy(p, 2, c).wait_recv()
        return stream[wide(c), :] + (near + xrec[p, wide(c)].astype(F32))

    def turn(p):
        for c in range(CHUNKS):
            stream[wide(c), :] = rs_total(p, c)
            norm_own(p + 1, c)
            ag_start(p + 1, c)

    stream[...] = tok[...].astype(F32)
    norm_own(0, 0)
    pl.semaphore_wait(barrier, greets)
    ag_start(0, 0)
    for c in range(1, CHUNKS):
        norm_own(0, c)
        ag_start(0, c)

    sends = []
    for p in (0, 1):
        axis, plan = plans[p]
        n, m, unit, groups, low, fold, span = plan.n, plan.m, plan.unit, plan.u, plan.low, plan.q, plan.blocks
        here = lax.axis_index(axis)
        abuf, res = ((a0, res0), (a1, res1))[p]
        s1, r1, s2, r2 = ((s10, r10, s20, r20), (s11, r11, s21, r21))[p]
        ready(2 * p)

        def owner_of(b, j, m=m, low=low, span=span):
            return lax.rem(j, low) + m * lax.div(b, span)

        def place(j, unit=unit):
            return pl.ds(pl.multiple_of(j * unit, unit), unit)

        def unit_copy(b, j, p=p, axis=axis, low=low, fold=fold, span=span, here=here, abuf=abuf, s1=s1, r1=r1,
                      owner_of=owner_of, place=place):
            owner = owner_of(b, j)
            u = lax.rem(b, span) * fold + lax.div(j, low)
            return owner, u, remote_copy(
                pk.at[p, b, place(j)], abuf.at[u, here], s1.at[b, j], r1.at[u, here], axis, owner)

        def first(i, _, p=p, m=m, here=here, abuf=abuf, unit_copy=unit_copy, place=place):
            k, c = arrival(i)
            b = block_at(k)
            ag_wait(p, k, c)
            queries, key_rows, values = project(p, b, c)
            pk[p, b, wide(c), 0:aw] = queries
            pk[p, b, wide(c), aw:2 * aw] = key_rows
            pk[p, b, wide(c), 2 * aw:3 * aw] = values
            for at in range(m // CHUNKS):
                j = c * (m // CHUNKS) + at
                owner, u, copy = unit_copy(b, j)

                @pl.when(owner != here)
                def _():
                    copy.start()

                @pl.when(owner == here)
                def _():
                    abuf[u, here] = pk[p, b, place(j), :]
            return 0

        lax.fori_loop(0, steps, first, 0)

        size = n * unit
        if p == 0:
            line_of = lambda at: lax.div(lax.rem(at, unit), width)
        else:
            line_of = lambda at: lax.div(lax.rem(at, unit), per_frame) * width + lax.rem(at, width)
        mask = line_of(lax.broadcasted_iota(jnp.int32, (size, 1), 0)) == line_of(
            lax.broadcasted_iota(jnp.int32, (1, size), 1))

        def home(u, m=m, low=low, fold=fold, span=span, here=here):
            return lax.div(u, fold) + span * lax.div(here, m), lax.rem(here, low) + low * lax.rem(u, fold)

        def back_copy(u, other, p=p, axis=axis, res=res, s2=s2, r2=r2, home=home, place=place):
            b, j = home(u)
            return remote_copy(
                res.at[u, other], att.at[p, b, place(j)], s2.at[u, other], r2.at[b, j], axis, other)

        def second(i, _, p=p, axis=axis, n=n, unit=unit, fold=fold, span=span, here=here, abuf=abuf, res=res,
                   r1=r1, s1=s1, mask=mask, size=size, back_copy=back_copy, home=home, place=place):
            k, sub = arrival(i) if fold == CHUNKS else (lax.div(i, fold), lax.rem(i, fold))
            u = lax.rem(block_at(k), span) * fold + sub
            for step in range(1, n):
                source = lax.rem(here + step, n)
                remote_copy(abuf.at[u, source], abuf.at[u, source], s1.at[0, 0], r1.at[u, source],
                            axis, source).wait_recv()
            done = attend(
                abuf[u, :, :, 0:aw].reshape(size, aw),
                abuf[u, :, :, aw:2 * aw].reshape(size, aw),
                abuf[u, :, :, 2 * aw:3 * aw].reshape(size, aw),
                mask,
            )
            res[u] = done.reshape(n, unit, aw)
            for step in range(1, n):
                back_copy(u, lax.rem(here + step, n)).start()
            b, j = home(u)
            att[p, b, place(j)] = res[u, here]
            return 0

        lax.fori_loop(0, groups, second, 0)
        ready(2 * p + 1)

        def third(i, _, p=p, axis=axis, m=m, here=here, s2=s2, r2=r2, owner_of=owner_of, place=place):
            k, c = departure(i)
            b = block_at(k)
            for at in range(m // CHUNKS):
                j = c * (m // CHUNKS) + at
                owner = owner_of(b, j)

                @pl.when(owner != here)
                def _():
                    ref = att.at[p, b, place(j)]
                    remote_copy(ref, ref, s2.at[0, 0], r2.at[b, j], axis, owner).wait_recv()
            rs_put(p, k, c, dot(att[p, b, wide(c)], wo[p]))

            @pl.when(k == 2)
            def _():
                rs_combine(p, c)
            return 0

        lax.fori_loop(0, steps, third, 0)
        turn(p)

        def drain(unit_copy=unit_copy, back_copy=back_copy, n=n, m=m, groups=groups, here=here):
            for b in range(n_ta):
                for j in range(m):
                    owner, _, copy = unit_copy(b, j)

                    @pl.when(owner != here)
                    def _():
                        copy.wait_send()
            for u in range(groups):
                for step in range(1, n):
                    back_copy(u, lax.rem(here + step, n)).wait_send()

        sends.append(drain)

    p = 2
    some_frames = frames // CHUNKS
    ready(2 * p)

    def time_first(i, _):
        k, c = arrival(i)
        b = block_at(k)
        ag_wait(p, k, c)
        queries, key_rows, values = project(p, b, c)
        at = pl.ds(b * frames + c * some_frames, some_frames)
        pk2[at, :, 0:aw] = queries.reshape(some_frames, per_frame, aw)
        pk2[at, :, aw:2 * aw] = key_rows.reshape(some_frames, per_frame, aw)
        pk2[at, :, 2 * aw:3 * aw] = values.reshape(some_frames, per_frame, aw)
        return 0

    lax.fori_loop(0, steps, time_first, 0)
    every = n_ta * frames
    some = 16
    size = every * some
    i_at = lax.broadcasted_iota(jnp.int32, (size, 1), 0)
    j_at = lax.broadcasted_iota(jnp.int32, (1, size), 1)
    causal = (lax.rem(i_at, some) == lax.rem(j_at, some)) & (lax.div(i_at, some) >= lax.div(j_at, some))

    def time_second(g, _):
        at = pl.ds(pl.multiple_of(g * some, some), some)
        done = attend(
            pk2[:, at, 0:aw].reshape(size, aw),
            pk2[:, at, aw:2 * aw].reshape(size, aw),
            pk2[:, at, 2 * aw:3 * aw].reshape(size, aw),
            causal,
        )
        att2[:, at, :] = done.reshape(every, some, aw)
        return 0

    lax.fori_loop(0, per_frame // some, time_second, 0)
    ready(2 * p + 1)

    def time_third(i, _):
        k, c = departure(i)
        b = block_at(k)
        at = pl.ds(b * frames + c * some_frames, some_frames)
        rs_put(p, k, c, dot(att2[at].reshape(piece, aw), wo[p]))

        @pl.when(k == 2)
        def _():
            rs_combine(p, c)
        return 0

    lax.fori_loop(0, steps, time_third, 0)
    turn(p)

    ready(6)
    ready(7)
    half = wf.shape[0]

    def mlp(i, _):
        k, c = arrival(i)
        b = block_at(k)
        ag_wait(3, k, c)
        both = dot(gath[3, b, wide(c)], wi[...])
        gate, up = both[:, :half], both[:, half:]
        hidden = (gate / (1.0 + jnp.exp(-gate)) * up).astype(BF16)
        rs_put(3, k, c, dot(hidden, wf[...]))

        @pl.when((k == 2) & (c > 0))
        def _():
            rs_combine(3, c - 1)
        return 0

    lax.fori_loop(0, steps, mlp, 0)
    rs_combine(3, CHUNKS - 1)
    for c in range(CHUNKS):
        out[wide(c), :] = rs_total(3, c).astype(BF16)

    for drain in sends:
        drain()
    for p in range(4):
        for slot in range(3):
            for c in range(CHUNKS):
                ag_copy(p, slot, c).wait_send()
                rs_copy(p, slot, c).wait_send()


def general_local(sizes, tokens, norm_gain, qkv_weight, qk_gain, out_weight, ffn_in, ffn_out):
    n_ta, n_ha, n_wa = sizes
    extent = tokens.shape
    clips, frames, height, width, model = extent
    rows = clips * frames * height * width
    aw = qkv_weight.shape[-1]
    half = ffn_in.shape[-1]
    plans = (("wa", Plan(n_wa, n_ta, frames, rows)), ("ha", Plan(n_ha, n_ta, frames, rows)))
    cfg = (n_ta, frames, height, width, plans)
    heads = aw // HEAD_DIM
    gains = jnp.tile(qk_gain.reshape(-1, HEAD_DIM), (1, heads))
    dma = pltpu.SemaphoreType.DMA
    vm = pltpu.VMEM
    scratch = [
        vm((rows, model), F32),
        vm((4, n_ta, rows, model), BF16),
        vm((3, model, 3 * aw), BF16),
        vm((3, aw, model), BF16),
        vm((model, 2 * half), BF16),
        vm((half, model), BF16),
        vm((2, n_ta, rows, 3 * aw), BF16),
    ]
    for width_of in (3 * aw, aw):
        for _, plan in plans:
            scratch.append(vm((plan.u, plan.n, plan.unit, width_of), BF16))
    scratch += [
        vm((2, n_ta, rows, aw), BF16),
        vm((n_ta * frames, height * width, 3 * aw), BF16),
        vm((n_ta * frames, height * width, aw), BF16),
        vm((4, n_ta, rows, model), BF16),
        vm((4, 2, rows, model), BF16),
        vm((4, rows, model), BF16),
        vm((4, rows, model), BF16),
        dma((4, 4)),
        dma((4, 3, CHUNKS)),
        dma((4, 3, CHUNKS)),
    ]
    for _, plan in plans:
        scratch += [
            dma((n_ta, plan.m)),
            dma((plan.u, plan.n)),
            dma((plan.u, plan.n)),
            dma((n_ta, plan.m)),
        ]
    scratch += [dma((4, 3, CHUNKS)), dma((4, 3, CHUNKS))]
    vmem = pl.BlockSpec(memory_space=pltpu.VMEM)
    anyw = pl.BlockSpec(memory_space=pl.ANY)
    result = pl.pallas_call(
        functools.partial(general_kernel, cfg),
        out_shape=jax.ShapeDtypeStruct((rows, model), BF16),
        in_specs=[vmem, vmem, vmem, anyw, anyw, anyw, anyw],
        out_specs=vmem,
        scratch_shapes=scratch,
        compiler_params=pltpu.CompilerParams(
            collective_id=0, has_side_effects=True, vmem_limit_bytes=67043328),
        name="axial_layer",
    )(
        tokens.reshape(rows, model),
        norm_gain,
        gains,
        jnp.transpose(qkv_weight, (0, 2, 1, 3)),
        out_weight,
        ffn_in.reshape(model, 2 * half),
        ffn_out,
    )
    return result.reshape(extent)


def axial_kernel(cfg, tok, gain, qkg, wq_h, wo_h, wi_h, wf_h, out, *s):
    n_ta, n_ha, n_wa, frames, height, width = cfg
    (x0, stream, gath, wq, wo, wi, wf, wi_far, wf_far, sx1, x1, pk2, att2, pbuf, prec, comb, xrec, fo, ro,
     wsem, x0_s, x0_r, ag_s, ag_r, rs_s, rs_r, x1_s, x1_r, fo_s, fo_r,
     wx_s, wx_r, wz_s, wz_r, wy_s, wy_r) = s
    model = tok.shape[-1]
    aw = wo.shape[1]
    piece = frames * height * width // CHUNKS
    some_frames = frames // CHUNKS
    sub_rows = height // n_wa
    sub_cols = width // n_ha
    spots = sub_rows * sub_cols
    unit = some_frames * spots
    groups = n_ha * n_wa
    some_groups = groups // CHUNKS
    some_wa = n_wa // CHUNKS
    me = lax.axis_index("ta")
    at_ha = lax.axis_index("ha")
    at_wa = lax.axis_index("wa")
    here = at_wa * n_ha + at_ha
    core, chip = lax.rem(me, 2), lax.div(me, 2)

    def block_at(k):
        return lax.rem(chip + lax.div(k, 2), 2) * 2 + lax.rem(core + lax.rem(k, 2), 2)

    partner = block_at(1)
    remote = block_at(2)
    steps = n_ta * CHUNKS
    early = 2 * CHUNKS

    def arrival(i):
        late = i - early
        c = jnp.where(i < early, lax.div(i, 2), lax.div(late, 2))
        k = jnp.where(i < early, lax.rem(i, 2), 2 + lax.rem(late, 2))
        return k, c

    copies = []
    for at in range(3):
        copies.append([
            pltpu.make_async_copy(wq_h.at[at, j], wq.at[at, :, j * aw:(j + 1) * aw], wsem.at[at, j])
            for j in range(3)])
        copies.append([pltpu.make_async_copy(wo_h.at[at], wo.at[at], wsem.at[at, 3])])
    copies.append([pltpu.make_async_copy(wi_h, wi, wsem.at[3, 0])])
    copies.append([pltpu.make_async_copy(wf_h, wf, wsem.at[3, 1])])

    def ready(at):
        for copy in copies[at]:
            copy.wait()

    barrier = pltpu.get_barrier_semaphore()
    for other in (partner, remote):
        pl.semaphore_signal(barrier, inc=1, device_id={"ta": other}, device_id_type=MESH)

    def group_place(g):
        return {"wa": lax.div(g, n_ha), "ha": lax.rem(g, n_ha)}

    for step in range(1, groups):
        pl.semaphore_signal(barrier, inc=1, device_id=group_place(lax.rem(here + step, groups)), device_id_type=MESH)
    greets = groups + 1

    def remote_copy(src, dst, send, recv, place):
        return pltpu.make_async_remote_copy(
            src_ref=src, dst_ref=dst, send_sem=send, recv_sem=recv,
            device_id=place, device_id_type=MESH)

    for group in copies:
        for copy in group:
            copy.start()

    def x0_copy(c, source, target):
        at = pl.ds(c * some_frames, some_frames)
        return remote_copy(tok.at[at, target], x0.at[at, source], x0_s.at[c, target], x0_r.at[c, source],
                           {"wa": target})

    far_pairs = ((wi_h, wi_far), (wf_h, wf_far))

    def far_x(j):
        src, dst = far_pairs[j]
        size = dst.shape[2]
        at = pl.ds(pl.multiple_of(here * size, size), size)
        return remote_copy(src.at[at], dst.at[at_wa, at_ha], wx_s.at[j], wx_r.at[j], {"ta": remote})

    def far_z(j, source, target):
        ref = far_pairs[j][1].at[at_wa, source]
        return remote_copy(ref, ref, wz_s.at[j, target], wz_r.at[j, source], {"ha": target})

    def far_y(j, wa_source, part, target):
        ref = far_pairs[j][1].at[wa_source, part]
        return remote_copy(ref, ref, wy_s.at[j, target, part], wy_r.at[j, wa_source, part], {"wa": target})

    def far_spread(part):
        for j in range(2):
            for step in range(1, n_wa):
                far_y(j, at_wa, part, lax.rem(at_wa + step, n_wa)).start()

    def far_first():
        for j in range(2):
            far_x(j).wait_recv()
            for step in range(1, n_ha):
                far_z(j, at_ha, lax.rem(at_ha + step, n_ha)).start()
        far_spread(at_ha)

    def far_next(step):
        source = lax.rem(at_ha + step, n_ha)
        for j in range(2):
            far_z(j, source, source).wait_recv()
        far_spread(source)

    def far_ready():
        for j in range(2):
            for step in range(1, n_wa):
                source = lax.rem(at_wa + step, n_wa)
                for part in range(n_ha):
                    far_y(j, source, part, source).wait_recv()

    def norm_own(p, c):
        x = stream[p // 2, c]
        scale = lax.rsqrt(jnp.mean(x * x, axis=-1, keepdims=True) + EPS)
        gath[p, me, c] = (x * scale * gain[p:p + 1, :]).astype(BF16)

    def ag_copy(p, slot, c):
        block = me if slot < 2 else remote
        other = remote if slot == 1 else partner
        ref = gath.at[p, block, c]
        return remote_copy(ref, ref, ag_s.at[p, slot, c], ag_r.at[p, slot, c], {"ta": other})

    def ag_start(p, c):
        ag_copy(p, 1, c).start()
        ag_copy(p, 0, c).start()

    def ag_wait(p, k, c):
        @pl.when(k == 1)
        def _():
            ag_copy(p, 0, c).wait_recv()

        @pl.when(k == 2)
        def _():
            ag_copy(p, 1, c).wait_recv()
            ag_copy(p, 2, c).start()

        @pl.when(k == 3)
        def _():
            ag_copy(p, 2, c).wait_recv()

    lane_a = lax.broadcasted_iota(jnp.int32, (aw, aw), 0) // HEAD_DIM
    lane_b = lax.broadcasted_iota(jnp.int32, (aw, aw), 1) // HEAD_DIM
    ones = (lane_a == lane_b).astype(F32).astype(BF16)

    def head_norm(x, row):
        square = x * x
        high = square.astype(BF16)
        low = (square - high.astype(F32)).astype(BF16)
        mean = (dot(high, ones) + dot(low, ones)) * (1.0 / HEAD_DIM)
        return x * lax.rsqrt(mean + EPS) * qkg[row:row + 1, :]

    def project(p, b, c):
        flat = dot(gath[p, b, c], wq[p])
        queries = (head_norm(flat[:, :aw], 2 * p) * (HEAD_DIM ** -0.5)).astype(BF16)
        key_rows = head_norm(flat[:, aw:2 * aw], 2 * p + 1).astype(BF16)
        return queries, key_rows, flat[:, 2 * aw:].astype(BF16)

    def rs_copy(p, slot, c):
        send, recv = rs_s.at[p, slot, c], rs_r.at[p, slot, c]
        if slot == 2:
            return remote_copy(comb.at[p, c], xrec.at[p, c], send, recv, {"ta": remote})
        return remote_copy(pbuf.at[p, 2 * slot + 1, c], prec.at[p, slot, c], send, recv, {"ta": partner})

    def rs_put(p, k, c, part):
        pbuf[p, k, c] = part.astype(BF16)

        @pl.when(k == 1)
        def _():
            rs_copy(p, 0, c).start()

        @pl.when(k == 3)
        def _():
            rs_copy(p, 1, c).start()

    def rs_combine(p, c):
        rs_copy(p, 1, c).wait_recv()
        comb[p, c] = (pbuf[p, 2, c].astype(F32) + prec[p, 1, c].astype(F32)).astype(BF16)
        rs_copy(p, 2, c).start()

    def rs_near(p, c):
        rs_copy(p, 0, c).wait_recv()
        return pbuf[p, 0, c].astype(F32) + prec[p, 0, c].astype(F32)

    def rs_total(p, c):
        near = rs_near(p, c)
        rs_copy(p, 2, c).wait_recv()
        return stream[p // 2, c] + (near + xrec[p, c].astype(F32))

    def pick_rows(source):
        return (source == lax.broadcasted_iota(jnp.int32, (1, piece), 1)).astype(F32).astype(BF16)

    index = lax.broadcasted_iota(jnp.int32, (piece, 1), 0)

    def digits(value, sizes):
        found = []
        for size in sizes[::-1]:
            found.append(lax.rem(value, size))
            value = lax.div(value, size)
        return found[::-1]

    def number(parts, sizes):
        value = parts[0]
        for part, size in zip(parts[1:], sizes[1:]):
            value = value * size + part
        return value

    def x1_copy(c, source, target):
        return remote_copy(sx1.at[c, target], x1.at[c, source], x1_s.at[c, target], x1_r.at[c, source],
                           group_place(target))

    def x1_send(c):
        w, h, f, r, q = digits(index, (n_wa, n_ha, some_frames, sub_rows, sub_cols))
        source = number((f, w, r, h, q), (some_frames, n_wa, sub_rows, n_ha, sub_cols))
        moved = dot(pick_rows(source), rs_total(0, c).astype(BF16)).astype(BF16)
        sx1[c] = moved.reshape(groups, unit, model)
        for step in range(1, groups):
            x1_copy(c, here, lax.rem(here + step, groups)).start()
        x1[c, here] = sx1[c, here]

    def x1_take(c):
        for step in range(1, groups):
            source = lax.rem(here + step, groups)
            x1_copy(c, source, source).wait_recv()
        stream[0, c] = x1[c].reshape(piece, model).astype(F32)
        norm_own(1, c)
        ag_start(1, c)

    def fo_copy(c, source, target):
        return remote_copy(fo.at[c, :, :, target], ro.at[c, source], fo_s.at[c, target], fo_r.at[c, source],
                           {"ha": target})

    def fo_send(c):
        near = rs_near(3, c)
        total = (stream[1, c] + near).astype(BF16)
        fo[c] = total.reshape(CHUNKS, some_wa, n_ha, unit, model)
        for step in range(1, n_ha):
            fo_copy(c, at_ha, lax.rem(at_ha + step, n_ha)).start()
        ro[c, at_ha] = fo[c, :, :, at_ha]

    def fo_take(c):
        for step in range(1, n_ha):
            source = lax.rem(at_ha + step, n_ha)
            fo_copy(c, source, source).wait_recv()
        f0, f1, w, r, h, q = digits(index, (CHUNKS, some_frames, some_wa, sub_rows, n_ha, sub_cols))
        source = number((h, f0, w, f1, r, q), (n_ha, CHUNKS, some_wa, some_frames, sub_rows, sub_cols))
        moved = dot(pick_rows(source), ro[c].reshape(piece, model)).astype(BF16)
        out[:, c * some_wa:(c + 1) * some_wa] = moved.reshape(frames, some_wa, sub_rows * width, model)

    x0[:, at_wa] = tok[:, at_wa]
    pl.semaphore_wait(barrier, greets)
    for c in range(CHUNKS):
        for step in range(1, n_wa):
            x0_copy(c, at_wa, lax.rem(at_wa + step, n_wa)).start()
    for j in range(2):
        far_x(j).start()
    for c in range(CHUNKS):
        for step in range(1, n_wa):
            source = lax.rem(at_wa + step, n_wa)
            x0_copy(c, source, source).wait_recv()
        stream[0, c] = x0[c * some_frames:(c + 1) * some_frames].reshape(piece, model).astype(F32)
        norm_own(0, c)
        ag_start(0, c)

    column = lax.broadcasted_iota(jnp.int32, (1, piece), 1)

    def lines_0(at):
        f, w, r, q = digits(at, (some_frames, n_wa, sub_rows, width))
        return f * sub_rows + r

    def lines_1(at):
        g, f, r, q = digits(at, (groups, some_frames, sub_rows, sub_cols))
        return f * sub_cols + q

    def line_step(p, i, mask):
        k, c = arrival(i)
        b = block_at(k)
        ag_wait(p, k, c)
        queries, key_rows, values = project(p, b, c)
        rs_put(p, k, c, dot(attend(queries, key_rows, values, mask), wo[p]))

        @pl.when((k == 2) & (c > 0))
        def _():
            rs_combine(p, c - 1)

    ready(0)
    ready(1)
    mask_0 = lines_0(index) == lines_0(column)

    def pass_0(i, _):
        line_step(0, i, mask_0)
        return 0

    lax.fori_loop(0, steps, pass_0, 0)
    rs_combine(0, CHUNKS - 1)
    far_first()
    x1_send(0)
    x1_take(0)
    ready(2)
    ready(3)
    mask_1 = lines_1(index) == lines_1(column)

    def pass_1(i, _):
        for c in range(1, CHUNKS):
            @pl.when(i == 2 * c - 1)
            def _():
                x1_send(c)

            @pl.when(i == 2 * c)
            def _():
                x1_take(c)

        line_step(1, i, mask_1)
        return 0

    lax.fori_loop(0, steps, pass_1, 0)
    rs_combine(1, CHUNKS - 1)
    far_next(1)

    half_piece = piece // CHUNKS
    for c in range(CHUNKS):
        total = rs_total(1, c)
        for d in range(CHUNKS):
            stream[1, d, c * half_piece:(c + 1) * half_piece] = total[d * half_piece:(d + 1) * half_piece]
    for d in range(CHUNKS):
        norm_own(2, d)
        ag_start(2, d)

    for at in (4, 5):
        ready(at)
    for step in range(2, n_ha):
        far_next(step)
    t_i = lax.div(index, unit) * some_frames + lax.div(lax.rem(index, unit), spots)
    t_j = lax.div(column, unit) * some_frames + lax.div(lax.rem(column, unit), spots)
    causal = (lax.rem(index, spots) == lax.rem(column, spots)) & (t_i >= t_j)

    def time_project(i, _):
        k, c = arrival(i)
        b = block_at(k)
        ag_wait(2, k, c)
        queries, key_rows, values = project(2, b, c)
        pk2[c, b, :, :, :, 0:aw] = queries.reshape(CHUNKS, some_groups, unit, aw)
        pk2[c, b, :, :, :, aw:2 * aw] = key_rows.reshape(CHUNKS, some_groups, unit, aw)
        pk2[c, b, :, :, :, 2 * aw:3 * aw] = values.reshape(CHUNKS, some_groups, unit, aw)
        return 0

    def time_attend(i, _):
        c = lax.div(i, some_groups)
        g = lax.rem(i, some_groups)
        done = attend(
            pk2[c, :, :, g, :, 0:aw].reshape(piece, aw),
            pk2[c, :, :, g, :, aw:2 * aw].reshape(piece, aw),
            pk2[c, :, :, g, :, 2 * aw:3 * aw].reshape(piece, aw),
            causal,
        )
        att2[c, :, :, g] = done.reshape(n_ta, CHUNKS, unit, aw)
        return 0

    def time_out(i, _):
        c = lax.div(i, n_ta)
        k = 3 - lax.rem(i, n_ta)
        b = block_at(k)
        rs_put(2, k, c, dot(att2[c, b].reshape(piece, aw), wo[2]))

        @pl.when(k == 1)
        def _():
            rs_combine(2, c)
        return 0

    lax.fori_loop(0, early, time_project, 0)

    def time_chunk(c, _):
        lax.fori_loop(early + 2 * c, early + 2 * c + 2, time_project, 0)
        lax.fori_loop(c * some_groups, (c + 1) * some_groups, time_attend, 0)
        lax.fori_loop(c * n_ta, (c + 1) * n_ta, time_out, 0)
        return 0

    lax.fori_loop(0, CHUNKS, time_chunk, 0)

    for at in (6, 7):
        ready(at)
    far_ready()
    half = wf.shape[0]

    def silu_part(x, w_in, w_out):
        both = dot(x, w_in)
        gate, up = both[:, :half], both[:, half:]
        hidden = (gate / (1.0 + jnp.exp(-gate)) * up).astype(BF16)
        return dot(hidden, w_out)

    def mlp(i, _):
        k, c = lax.rem(i, 2), lax.div(i, 2)
        b = block_at(k)

        for d in range(CHUNKS):
            @pl.when(i == 2 * d)
            def _():
                stream[1, d] = rs_total(2, d)
                norm_own(3, d)
                ag_copy(3, 0, d).start()

        @pl.when(k == 1)
        def _():
            ag_copy(3, 0, c).wait_recv()

        x = gath[3, b, c]
        part = silu_part(x, wi[...], wf[...]) + silu_part(
            x, wi_far[...].reshape(model, 2 * half), wf_far[...].reshape(half, model))
        pbuf[3, k, c] = part.astype(BF16)

        @pl.when(k == 1)
        def _():
            rs_copy(3, 0, c).start()

        return 0

    lax.fori_loop(0, 2 * CHUNKS, mlp, 0)
    for c in range(CHUNKS):
        fo_send(c)
    for c in range(CHUNKS):
        fo_take(c)

    for c in range(CHUNKS):
        for step in range(1, n_wa):
            x0_copy(c, at_wa, lax.rem(at_wa + step, n_wa)).wait_send()
        for step in range(1, groups):
            x1_copy(c, here, lax.rem(here + step, groups)).wait_send()
        for step in range(1, n_ha):
            fo_copy(c, at_ha, lax.rem(at_ha + step, n_ha)).wait_send()
        for p in range(3):
            for slot in range(3):
                ag_copy(p, slot, c).wait_send()
                rs_copy(p, slot, c).wait_send()
        ag_copy(3, 0, c).wait_send()
        rs_copy(3, 0, c).wait_send()
    for j in range(2):
        far_x(j).wait_send()
        for step in range(1, n_ha):
            far_z(j, at_ha, lax.rem(at_ha + step, n_ha)).wait_send()
        for step in range(1, n_wa):
            for part in range(n_ha):
                far_y(j, at_wa, part, lax.rem(at_wa + step, n_wa)).wait_send()


def axial_local(sizes, tokens, norm_gain, qkv_weight, qk_gain, out_weight, ffn_in, ffn_out):
    n_ta, n_ha, n_wa = sizes
    extent = tokens.shape
    clips, frames, height, width, model = extent
    frames = clips * frames
    rows = frames * height * width
    piece = rows // CHUNKS
    aw = qkv_weight.shape[-1]
    half = ffn_in.shape[-1]
    groups = n_ha * n_wa
    unit = piece // groups
    sub = height // n_wa * width
    heads = aw // HEAD_DIM
    gains = jnp.tile(qk_gain.reshape(-1, HEAD_DIM), (1, heads))
    dma = pltpu.SemaphoreType.DMA
    vm = pltpu.VMEM
    scratch = [
        vm((frames, n_wa, sub, model), BF16),
        vm((2, CHUNKS, piece, model), F32),
        vm((4, n_ta, CHUNKS, piece, model), BF16),
        vm((3, model, 3 * aw), BF16),
        vm((3, aw, model), BF16),
        vm((model, 2 * half), BF16),
        vm((half, model), BF16),
        vm((n_wa, n_ha, model // groups, 2 * half), BF16),
        vm((n_wa, n_ha, half // groups, model), BF16),
        vm((CHUNKS, groups, unit, model), BF16),
        vm((CHUNKS, groups, unit, model), BF16),
        vm((CHUNKS, n_ta, CHUNKS, groups // CHUNKS, unit, 3 * aw), BF16),
        vm((CHUNKS, n_ta, CHUNKS, groups // CHUNKS, unit, aw), BF16),
        vm((4, n_ta, CHUNKS, piece, model), BF16),
        vm((4, 2, CHUNKS, piece, model), BF16),
        vm((3, CHUNKS, piece, model), BF16),
        vm((3, CHUNKS, piece, model), BF16),
        vm((CHUNKS, CHUNKS, n_wa // CHUNKS, n_ha, unit, model), BF16),
        vm((CHUNKS, n_ha, CHUNKS, n_wa // CHUNKS, unit, model), BF16),
        dma((4, 4)),
        dma((CHUNKS, n_wa)),
        dma((CHUNKS, n_wa)),
        dma((4, 3, CHUNKS)),
        dma((4, 3, CHUNKS)),
        dma((4, 3, CHUNKS)),
        dma((4, 3, CHUNKS)),
        dma((CHUNKS, groups)),
        dma((CHUNKS, groups)),
        dma((CHUNKS, n_ha)),
        dma((CHUNKS, n_ha)),
        dma((2,)),
        dma((2,)),
        dma((2, n_ha)),
        dma((2, n_ha)),
        dma((2, n_wa, n_ha)),
        dma((2, n_wa, n_ha)),
    ]
    vmem = pl.BlockSpec(memory_space=pltpu.VMEM)
    anyw = pl.BlockSpec(memory_space=pl.ANY)
    result = pl.pallas_call(
        functools.partial(axial_kernel, (n_ta, n_ha, n_wa, frames, height, width)),
        out_shape=jax.ShapeDtypeStruct((frames, n_wa, sub, model), BF16),
        in_specs=[vmem, vmem, vmem, anyw, anyw, anyw, anyw],
        out_specs=vmem,
        scratch_shapes=scratch,
        compiler_params=pltpu.CompilerParams(
            collective_id=0, has_side_effects=True, vmem_limit_bytes=67043328),
        name="axial_layer",
    )(
        tokens.reshape(frames, n_wa, sub, model),
        norm_gain,
        gains,
        jnp.transpose(qkv_weight, (0, 2, 1, 3)),
        out_weight,
        ffn_in.reshape(model, 2 * half),
        ffn_out,
    )
    return result.reshape(extent)


def local(sizes, tokens, *weights):
    n_ta, n_ha, n_wa = sizes
    clips, frames, height, width, _ = tokens.shape
    fits = n_wa % CHUNKS == 0 and height % n_wa == 0 and width % n_ha == 0 and clips * frames % CHUNKS == 0
    unit = clips * frames * height * width // (CHUNKS * n_ha * n_wa)
    if fits and unit % 16 == 0:
        return axial_local(sizes, tokens, *weights)
    return general_local(sizes, tokens, *weights)


def solution(mesh):
    sizes = tuple(mesh.shape[name] for name in ("ta", "ha", "wa"))
    return jax.shard_map(
        functools.partial(local, sizes),
        mesh=mesh,
        in_specs=(
            P(None, "ta", "ha", "wa", None),
            P(),
            P(None, None, None, "ta"),
            P(),
            P(None, "ta", None),
            P(None, None, "ta"),
            P("ta", None),
        ),
        out_specs=P(None, "ta", "ha", "wa", None),
        check_vma=False,
    )
```

```python
import functools

import jax
import jax.numpy as jnp
from jax import lax
from jax.experimental import pallas as pl
from jax.experimental.pallas import tpu as pltpu
from jax.sharding import PartitionSpec as P

HEAD_DIM = 64
CHUNKS = 2
EPS = 1e-06
MESH = pl.DeviceIdType.MESH
F32 = jnp.float32
BF16 = jnp.bfloat16


def dot(a, b):
    return jnp.dot(a, b, preferred_element_type=F32)


def dot_t(a, b):
    return lax.dot_general(a, b, (((1,), (1,)), ((), ())), preferred_element_type=F32)


def attend(queries, key_rows, values, mask):
    width = queries.shape[-1]
    lane_head = lax.broadcasted_iota(jnp.int32, (1, width), 1) // HEAD_DIM
    total = None
    for head in range(width // HEAD_DIM):
        pick = (lane_head == head).astype(F32).astype(BF16)
        scores = dot_t(queries * pick, key_rows)
        weights = jnp.where(mask, jnp.exp(scores), 0.0)
        probs = weights * (1.0 / jnp.sum(weights, axis=-1, keepdims=True))
        part = dot(probs.astype(BF16), values * pick)
        total = part if total is None else total + part
    return total.astype(BF16)


class Plan:
    def __init__(self, n, n_ta, frames, rows):
        self.n = n
        self.m = frames
        self.unit = rows // frames
        self.low = min(n, frames)
        self.q = frames // self.low
        self.blocks = n_ta * frames // max(n, frames)
        self.u = self.blocks * self.q


def general_kernel(cfg, tok, gain, qkg, wq_h, wo_h, wi_h, wf_h, out, *s):
    n_ta, frames, height, width, plans = cfg
    (stream, gath, wq, wo, wi, wf, pk, a0, a1, res0, res1, att, pk2, att2, pbuf, prec, comb, xrec,
     wsem, ag_s, ag_r, s10, r10, s20, r20, s11, r11, s21, r21, rs_s, rs_r) = s
    rows = tok.shape[0]
    per_frame = height * width
    aw = wo.shape[1]
    me = lax.axis_index("ta")
    core, chip = lax.rem(me, 2), lax.div(me, 2)

    def block_at(k):
        return lax.rem(chip + lax.div(k, 2), 2) * 2 + lax.rem(core + lax.rem(k, 2), 2)

    piece = rows // CHUNKS
    wide = lambda c: pl.ds(pl.multiple_of(c * piece, piece), piece)
    steps = n_ta * CHUNKS
    early = 2 * CHUNKS

    def arrival(i):
        late = i - early
        k = jnp.where(i < early, lax.div(i, CHUNKS), 2 + lax.rem(late, 2))
        c = jnp.where(i < early, lax.rem(i, CHUNKS), lax.div(late, 2))
        return k, c

    def departure(i):
        rest = i - early
        k = jnp.where(i < early, 3 - lax.rem(i, 2), 1 - lax.div(rest, CHUNKS))
        c = jnp.where(i < early, lax.div(i, 2), lax.rem(rest, CHUNKS))
        return k, c

    partner = block_at(1)
    remote = block_at(2)
    pair_last = block_at(3)

    copies = []
    for at in range(3):
        copies.append([
            pltpu.make_async_copy(wq_h.at[at, j], wq.at[at, :, j * aw:(j + 1) * aw], wsem.at[at, j])
            for j in range(3)])
        copies.append([pltpu.make_async_copy(wo_h.at[at], wo.at[at], wsem.at[at, 3])])
    copies.append([pltpu.make_async_copy(wi_h, wi, wsem.at[3, 0])])
    copies.append([pltpu.make_async_copy(wf_h, wf, wsem.at[3, 1])])
    for group in copies:
        for copy in group:
            copy.start()

    def ready(at):
        for copy in copies[at]:
            copy.wait()

    barrier = pltpu.get_barrier_semaphore()
    greets = 0
    for other in (partner, remote):
        pl.semaphore_signal(barrier, inc=1, device_id={"ta": other}, device_id_type=MESH)
        greets += 1
    for axis, plan in plans:
        here = lax.axis_index(axis)
        for step in range(1, plan.n):
            other = lax.rem(here + step, plan.n)
            pl.semaphore_signal(barrier, inc=1, device_id={axis: other}, device_id_type=MESH)
            greets += 1

    def remote_copy(src, dst, send, recv, axis, other):
        return pltpu.make_async_remote_copy(
            src_ref=src, dst_ref=dst, send_sem=send, recv_sem=recv,
            device_id={axis: other}, device_id_type=MESH)

    def norm_own(p, c):
        x = stream[wide(c), :]
        scale = lax.rsqrt(jnp.mean(x * x, axis=-1, keepdims=True) + EPS)
        gath[p, me, wide(c)] = (x * scale * gain[p:p + 1, :]).astype(BF16)

    def ag_copy(p, slot, c):
        block = me if slot < 2 else remote
        other = remote if slot == 1 else partner
        ref = gath.at[p, block, wide(c)]
        return remote_copy(ref, ref, ag_s.at[p, slot, c], ag_r.at[p, slot, c], "ta", other)

    def ag_start(p, c):
        ag_copy(p, 1, c).start()
        ag_copy(p, 0, c).start()

    def ag_wait(p, k, c):
        @pl.when(k == 1)
        def _():
            ag_copy(p, 0, c).wait_recv()

        @pl.when(k == 2)
        def _():
            ag_copy(p, 1, c).wait_recv()
            ag_copy(p, 2, c).start()

        @pl.when(k == 3)
        def _():
            ag_copy(p, 2, c).wait_recv()

    lane_a = lax.broadcasted_iota(jnp.int32, (aw, aw), 0) // HEAD_DIM
    lane_b = lax.broadcasted_iota(jnp.int32, (aw, aw), 1) // HEAD_DIM
    ones = (lane_a == lane_b).astype(F32).astype(BF16)

    def head_norm(x, row):
        square = x * x
        high = square.astype(BF16)
        low = (square - high.astype(F32)).astype(BF16)
        mean = (dot(high, ones) + dot(low, ones)) * (1.0 / HEAD_DIM)
        return x * lax.rsqrt(mean + EPS) * qkg[row:row + 1, :]

    def project(p, b, c):
        flat = dot(gath[p, b, wide(c)], wq[p])
        queries = (head_norm(flat[:, :aw], 2 * p) * (HEAD_DIM ** -0.5)).astype(BF16)
        key_rows = head_norm(flat[:, aw:2 * aw], 2 * p + 1).astype(BF16)
        return queries, key_rows, flat[:, 2 * aw:].astype(BF16)

    def rs_copy(p, slot, c):
        send, recv = rs_s.at[p, slot, c], rs_r.at[p, slot, c]
        if slot == 2:
            return remote_copy(comb.at[p, wide(c)], xrec.at[p, wide(c)], send, recv, "ta", remote)
        return remote_copy(pbuf.at[p, 2 * slot + 1, wide(c)], prec.at[p, slot, wide(c)], send, recv, "ta", partner)

    def rs_put(p, k, c, part):
        pbuf[p, k, wide(c)] = part.astype(BF16)

        @pl.when(k == 1)
        def _():
            rs_copy(p, 0, c).start()

        @pl.when(k == 3)
        def _():
            rs_copy(p, 1, c).start()

    def rs_combine(p, c):
        rs_copy(p, 1, c).wait_recv()
        comb[p, wide(c)] = (pbuf[p, 2, wide(c)].astype(F32) + prec[p, 1, wide(c)].astype(F32)).astype(BF16)
        rs_copy(p, 2, c).start()

    def rs_total(p, c):
        rs_copy(p, 0, c).wait_recv()
        near = pbuf[p, 0, wide(c)].astype(F32) + prec[p, 0, wide(c)].astype(F32)
        rs_copy(p, 2, c).wait_recv()
        return stream[wide(c), :] + (near + xrec[p, wide(c)].astype(F32))

    def turn(p):
        for c in range(CHUNKS):
            stream[wide(c), :] = rs_total(p, c)
            norm_own(p + 1, c)
            ag_start(p + 1, c)

    stream[...] = tok[...].astype(F32)
    norm_own(0, 0)
    pl.semaphore_wait(barrier, greets)
    ag_start(0, 0)
    for c in range(1, CHUNKS):
        norm_own(0, c)
        ag_start(0, c)

    sends = []
    for p in (0, 1):
        axis, plan = plans[p]
        n, m, unit, groups, low, fold, span = plan.n, plan.m, plan.unit, plan.u, plan.low, plan.q, plan.blocks
        here = lax.axis_index(axis)
        abuf, res = ((a0, res0), (a1, res1))[p]
        s1, r1, s2, r2 = ((s10, r10, s20, r20), (s11, r11, s21, r21))[p]
        ready(2 * p)

        def owner_of(b, j, m=m, low=low, span=span):
            return lax.rem(j, low) + m * lax.div(b, span)

        def place(j, unit=unit):
            return pl.ds(pl.multiple_of(j * unit, unit), unit)

        def unit_copy(b, j, p=p, axis=axis, low=low, fold=fold, span=span, here=here, abuf=abuf, s1=s1, r1=r1,
                      owner_of=owner_of, place=place):
            owner = owner_of(b, j)
            u = lax.rem(b, span) * fold + lax.div(j, low)
            return owner, u, remote_copy(
                pk.at[p, b, place(j)], abuf.at[u, here], s1.at[b, j], r1.at[u, here], axis, owner)

        def first(i, _, p=p, m=m, here=here, abuf=abuf, unit_copy=unit_copy, place=place):
            k, c = arrival(i)
            b = block_at(k)
            ag_wait(p, k, c)
            queries, key_rows, values = project(p, b, c)
            pk[p, b, wide(c), 0:aw] = queries
            pk[p, b, wide(c), aw:2 * aw] = key_rows
            pk[p, b, wide(c), 2 * aw:3 * aw] = values
            for at in range(m // CHUNKS):
                j = c * (m // CHUNKS) + at
                owner, u, copy = unit_copy(b, j)

                @pl.when(owner != here)
                def _():
                    copy.start()

                @pl.when(owner == here)
                def _():
                    abuf[u, here] = pk[p, b, place(j), :]
            return 0

        lax.fori_loop(0, steps, first, 0)

        size = n * unit
        if p == 0:
            line_of = lambda at: lax.div(lax.rem(at, unit), width)
        else:
            line_of = lambda at: lax.div(lax.rem(at, unit), per_frame) * width + lax.rem(at, width)
        mask = line_of(lax.broadcasted_iota(jnp.int32, (size, 1), 0)) == line_of(
            lax.broadcasted_iota(jnp.int32, (1, size), 1))

        def home(u, m=m, low=low, fold=fold, span=span, here=here):
            return lax.div(u, fold) + span * lax.div(here, m), lax.rem(here, low) + low * lax.rem(u, fold)

        def back_copy(u, other, p=p, axis=axis, res=res, s2=s2, r2=r2, home=home, place=place):
            b, j = home(u)
            return remote_copy(
                res.at[u, other], att.at[p, b, place(j)], s2.at[u, other], r2.at[b, j], axis, other)

        def second(i, _, p=p, axis=axis, n=n, unit=unit, fold=fold, span=span, here=here, abuf=abuf, res=res,
                   r1=r1, s1=s1, mask=mask, size=size, back_copy=back_copy, home=home, place=place):
            k, sub = arrival(i) if fold == CHUNKS else (lax.div(i, fold), lax.rem(i, fold))
            u = lax.rem(block_at(k), span) * fold + sub
            for step in range(1, n):
                source = lax.rem(here + step, n)
                remote_copy(abuf.at[u, source], abuf.at[u, source], s1.at[0, 0], r1.at[u, source],
                            axis, source).wait_recv()
            done = attend(
                abuf[u, :, :, 0:aw].reshape(size, aw),
                abuf[u, :, :, aw:2 * aw].reshape(size, aw),
                abuf[u, :, :, 2 * aw:3 * aw].reshape(size, aw),
                mask,
            )
            res[u] = done.reshape(n, unit, aw)
            for step in range(1, n):
                back_copy(u, lax.rem(here + step, n)).start()
            b, j = home(u)
            att[p, b, place(j)] = res[u, here]
            return 0

        lax.fori_loop(0, groups, second, 0)
        ready(2 * p + 1)

        def third(i, _, p=p, axis=axis, m=m, here=here, s2=s2, r2=r2, owner_of=owner_of, place=place):
            k, c = departure(i)
            b = block_at(k)
            for at in range(m // CHUNKS):
                j = c * (m // CHUNKS) + at
                owner = owner_of(b, j)

                @pl.when(owner != here)
                def _():
                    ref = att.at[p, b, place(j)]
                    remote_copy(ref, ref, s2.at[0, 0], r2.at[b, j], axis, owner).wait_recv()
            rs_put(p, k, c, dot(att[p, b, wide(c)], wo[p]))

            @pl.when(k == 2)
            def _():
                rs_combine(p, c)
            return 0

        lax.fori_loop(0, steps, third, 0)
        turn(p)

        def drain(unit_copy=unit_copy, back_copy=back_copy, n=n, m=m, groups=groups, here=here):
            for b in range(n_ta):
                for j in range(m):
                    owner, _, copy = unit_copy(b, j)

                    @pl.when(owner != here)
                    def _():
                        copy.wait_send()
            for u in range(groups):
                for step in range(1, n):
                    back_copy(u, lax.rem(here + step, n)).wait_send()

        sends.append(drain)

    p = 2
    some_frames = frames // CHUNKS
    ready(2 * p)

    def time_first(i, _):
        k, c = arrival(i)
        b = block_at(k)
        ag_wait(p, k, c)
        queries, key_rows, values = project(p, b, c)
        at = pl.ds(b * frames + c * some_frames, some_frames)
        pk2[at, :, 0:aw] = queries.reshape(some_frames, per_frame, aw)
        pk2[at, :, aw:2 * aw] = key_rows.reshape(some_frames, per_frame, aw)
        pk2[at, :, 2 * aw:3 * aw] = values.reshape(some_frames, per_frame, aw)
        return 0

    lax.fori_loop(0, steps, time_first, 0)
    every = n_ta * frames
    some = 16
    size = every * some
    i_at = lax.broadcasted_iota(jnp.int32, (size, 1), 0)
    j_at = lax.broadcasted_iota(jnp.int32, (1, size), 1)
    causal = (lax.rem(i_at, some) == lax.rem(j_at, some)) & (lax.div(i_at, some) >= lax.div(j_at, some))

    def time_second(g, _):
        at = pl.ds(pl.multiple_of(g * some, some), some)
        done = attend(
            pk2[:, at, 0:aw].reshape(size, aw),
            pk2[:, at, aw:2 * aw].reshape(size, aw),
            pk2[:, at, 2 * aw:3 * aw].reshape(size, aw),
            causal,
        )
        att2[:, at, :] = done.reshape(every, some, aw)
        return 0

    lax.fori_loop(0, per_frame // some, time_second, 0)
    ready(2 * p + 1)

    def time_third(i, _):
        k, c = departure(i)
        b = block_at(k)
        at = pl.ds(b * frames + c * some_frames, some_frames)
        rs_put(p, k, c, dot(att2[at].reshape(piece, aw), wo[p]))

        @pl.when(k == 2)
        def _():
            rs_combine(p, c)
        return 0

    lax.fori_loop(0, steps, time_third, 0)
    turn(p)

    ready(6)
    ready(7)
    half = wf.shape[0]

    def mlp(i, _):
        k, c = arrival(i)
        b = block_at(k)
        ag_wait(3, k, c)
        both = dot(gath[3, b, wide(c)], wi[...])
        gate, up = both[:, :half], both[:, half:]
        hidden = (gate / (1.0 + jnp.exp(-gate)) * up).astype(BF16)
        rs_put(3, k, c, dot(hidden, wf[...]))

        @pl.when((k == 2) & (c > 0))
        def _():
            rs_combine(3, c - 1)
        return 0

    lax.fori_loop(0, steps, mlp, 0)
    rs_combine(3, CHUNKS - 1)
    for c in range(CHUNKS):
        out[wide(c), :] = rs_total(3, c).astype(BF16)

    for drain in sends:
        drain()
    for p in range(4):
        for slot in range(3):
            for c in range(CHUNKS):
                ag_copy(p, slot, c).wait_send()
                rs_copy(p, slot, c).wait_send()


def general_local(sizes, tokens, norm_gain, qkv_weight, qk_gain, out_weight, ffn_in, ffn_out):
    n_ta, n_ha, n_wa = sizes
    extent = tokens.shape
    clips, frames, height, width, model = extent
    rows = clips * frames * height * width
    aw = qkv_weight.shape[-1]
    half = ffn_in.shape[-1]
    plans = (("wa", Plan(n_wa, n_ta, frames, rows)), ("ha", Plan(n_ha, n_ta, frames, rows)))
    cfg = (n_ta, frames, height, width, plans)
    heads = aw // HEAD_DIM
    gains = jnp.tile(qk_gain.reshape(-1, HEAD_DIM), (1, heads))
    dma = pltpu.SemaphoreType.DMA
    vm = pltpu.VMEM
    scratch = [
        vm((rows, model), F32),
        vm((4, n_ta, rows, model), BF16),
        vm((3, model, 3 * aw), BF16),
        vm((3, aw, model), BF16),
        vm((model, 2 * half), BF16),
        vm((half, model), BF16),
        vm((2, n_ta, rows, 3 * aw), BF16),
    ]
    for width_of in (3 * aw, aw):
        for _, plan in plans:
            scratch.append(vm((plan.u, plan.n, plan.unit, width_of), BF16))
    scratch += [
        vm((2, n_ta, rows, aw), BF16),
        vm((n_ta * frames, height * width, 3 * aw), BF16),
        vm((n_ta * frames, height * width, aw), BF16),
        vm((4, n_ta, rows, model), BF16),
        vm((4, 2, rows, model), BF16),
        vm((4, rows, model), BF16),
        vm((4, rows, model), BF16),
        dma((4, 4)),
        dma((4, 3, CHUNKS)),
        dma((4, 3, CHUNKS)),
    ]
    for _, plan in plans:
        scratch += [
            dma((n_ta, plan.m)),
            dma((plan.u, plan.n)),
            dma((plan.u, plan.n)),
            dma((n_ta, plan.m)),
        ]
    scratch += [dma((4, 3, CHUNKS)), dma((4, 3, CHUNKS))]
    vmem = pl.BlockSpec(memory_space=pltpu.VMEM)
    anyw = pl.BlockSpec(memory_space=pl.ANY)
    result = pl.pallas_call(
        functools.partial(general_kernel, cfg),
        out_shape=jax.ShapeDtypeStruct((rows, model), BF16),
        in_specs=[vmem, vmem, vmem, anyw, anyw, anyw, anyw],
        out_specs=vmem,
        scratch_shapes=scratch,
        compiler_params=pltpu.CompilerParams(
            collective_id=0, has_side_effects=True, vmem_limit_bytes=67043328),
        name="axial_layer",
    )(
        tokens.reshape(rows, model),
        norm_gain,
        gains,
        jnp.transpose(qkv_weight, (0, 2, 1, 3)),
        out_weight,
        ffn_in.reshape(model, 2 * half),
        ffn_out,
    )
    return result.reshape(extent)


def axial_kernel(cfg, tok, gain, qkg, wq_h, wo_h, wi_h, wf_h, out, *s):
    n_ta, n_ha, n_wa, frames, height, width = cfg
    (x0, stream, gath, wq, wo, wi, wf, wi_far, wf_far, sx1, x1, pk2, attb, att, pbuf, prec, fo, ro,
     wsem, x0_s, x0_r, ag_s, ag_r, rs_s, rs_r, at_s, at_r, x1_s, x1_r, fo_s, fo_r,
     wx_s, wx_r, wz_s, wz_r, wy_s, wy_r, wd_s, wd_r) = s
    model = tok.shape[-1]
    aw = pk2.shape[-1] // 3
    piece = frames * height * width // CHUNKS
    some_frames = frames // CHUNKS
    sub_rows = height // n_wa
    sub_cols = width // n_ha
    spots = sub_rows * sub_cols
    unit = some_frames * spots
    groups = n_ha * n_wa
    some_groups = groups // CHUNKS
    some_wa = n_wa // CHUNKS
    me = lax.axis_index("ta")
    at_ha = lax.axis_index("ha")
    at_wa = lax.axis_index("wa")
    here = at_wa * n_ha + at_ha
    core, chip = lax.rem(me, 2), lax.div(me, 2)

    def block_at(k):
        return lax.rem(chip + lax.div(k, 2), 2) * 2 + lax.rem(core + lax.rem(k, 2), 2)

    partner = block_at(1)
    remote = block_at(2)
    part_rows = piece // n_wa
    steps = n_ta * CHUNKS
    early = 2 * CHUNKS

    def arrival(i):
        late = i - early
        c = jnp.where(i < early, lax.div(i, 2), lax.div(late, 2))
        k = jnp.where(i < early, lax.rem(i, 2), 2 + lax.rem(late, 2))
        return k, c

    copies = []
    for at in range(3):
        copies.append([
            pltpu.make_async_copy(wq_h.at[at, j], wq.at[at, :, j * aw:(j + 1) * aw], wsem.at[at, j])
            for j in range(3)])
        copies.append([pltpu.make_async_copy(wo_h.at[at], wo.at[at, me], wsem.at[at, 3])])
    copies.append([pltpu.make_async_copy(wi_h, wi, wsem.at[3, 0])])
    copies.append([pltpu.make_async_copy(wf_h, wf, wsem.at[3, 1])])

    def ready(at):
        for copy in copies[at]:
            copy.wait()

    barrier = pltpu.get_barrier_semaphore()
    for other in (partner, remote):
        pl.semaphore_signal(barrier, inc=1, device_id={"ta": other}, device_id_type=MESH)

    def group_place(g):
        return {"wa": lax.div(g, n_ha), "ha": lax.rem(g, n_ha)}

    for step in range(1, groups):
        pl.semaphore_signal(barrier, inc=1, device_id=group_place(lax.rem(here + step, groups)), device_id_type=MESH)
    greets = groups + 1

    def remote_copy(src, dst, send, recv, place):
        return pltpu.make_async_remote_copy(
            src_ref=src, dst_ref=dst, send_sem=send, recv_sem=recv,
            device_id=place, device_id_type=MESH)

    for group in copies:
        for copy in group:
            copy.start()

    def x0_copy(c, source, target):
        at = pl.ds(c * some_frames, some_frames)
        return remote_copy(tok.at[at, target], x0.at[c, source], x0_s.at[c, target], x0_r.at[c, source],
                           {"wa": target})

    parts_in = wi_h.shape[0] // wi_far.shape[0]

    def far(j, shard):
        if j < 3:
            return wo.at[j, shard]
        return wi_far.at[j - 3] if j < 5 else wf_far

    def far_x(j):
        dst = far(j, me).at[at_wa, at_ha]
        if j < 3:
            src = wo_h.at[j, at_wa, at_ha]
        else:
            size = dst.shape[0]
            first = (j - 3) * parts_in if j < 5 else 0
            src = (wi_h if j < 5 else wf_h).at[pl.ds(pl.multiple_of(first + here * size, size), size)]
        return remote_copy(src, dst, wx_s.at[j], wx_r.at[j], {"ta": remote})

    def far_z(j, source, target):
        ref = far(j, remote).at[at_wa, source]
        return remote_copy(ref, ref, wz_s.at[j, target], wz_r.at[j, source], {"ha": target})

    def far_y(j, wa_source, part, target):
        ref = far(j, remote).at[wa_source, part]
        return remote_copy(ref, ref, wy_s.at[j, target, part], wy_r.at[j, wa_source, part], {"wa": target})

    def far_d(j, slot):
        if slot == 0:
            return remote_copy(wo_h.at[j], wo.at[j, me], wd_s.at[j, 0], wd_r.at[j, 0], {"ta": partner})
        ref = wo.at[j, remote]
        return remote_copy(ref, ref, wd_s.at[j, 1], wd_r.at[j, 1], {"ta": partner})

    def far_spread(j, part):
        for step in range(1, n_wa):
            far_y(j, at_wa, part, lax.rem(at_wa + step, n_wa)).start()

    def far_first(j):
        far_x(j).wait_recv()
        for step in range(1, n_ha):
            far_z(j, at_ha, lax.rem(at_ha + step, n_ha)).start()

    def far_own(j):
        far_spread(j, at_ha)

    def far_next(j):
        for step in range(1, n_ha):
            source = lax.rem(at_ha + step, n_ha)
            far_z(j, source, source).wait_recv()
            far_spread(j, source)

    def far_ready(j):
        for step in range(1, n_wa):
            source = lax.rem(at_wa + step, n_wa)
            for part in range(n_ha):
                far_y(j, source, part, source).wait_recv()

    def far_pair(j):
        far_ready(j)
        far_d(j, 1).start()

    def norm_rows(p, c, at):
        x = stream[p // 2, c, at]
        scale = lax.rsqrt(jnp.mean(x * x, axis=-1, keepdims=True) + EPS)
        gath[p, me, c, at] = (x * scale * gain[p:p + 1, :]).astype(BF16)

    def rows_of(part):
        start = part * part_rows
        return pl.ds(start if isinstance(part, int) else pl.multiple_of(start, part_rows), part_rows)

    def ag_copy(p, slot, c, part):
        block = me if slot < 2 else remote
        other = remote if slot == 1 else partner
        ref = gath.at[p, block, c, rows_of(part)]
        return remote_copy(ref, ref, ag_s.at[p, slot, c, part], ag_r.at[p, slot, c, part], {"ta": other})

    def ag_part(p, c, part):
        ag_copy(p, 1, c, part).start()
        ag_copy(p, 0, c, part).start()

    def norm_start(p, c):
        norm_rows(p, c, pl.ds(0, piece))
        for part in range(n_wa):
            ag_part(p, c, part)

    def ag_wait(p, k, c):
        @pl.when(k == 1)
        def _():
            for part in range(n_wa):
                ag_copy(p, 0, c, part).wait_recv()

        @pl.when(k == 2)
        def _():
            for part in range(n_wa):
                ag_copy(p, 1, c, part).wait_recv()
                ag_copy(p, 2, c, part).start()

        @pl.when(k == 3)
        def _():
            for part in range(n_wa):
                ag_copy(p, 2, c, part).wait_recv()

    lane_a = lax.broadcasted_iota(jnp.int32, (aw, aw), 0) // HEAD_DIM
    lane_b = lax.broadcasted_iota(jnp.int32, (aw, aw), 1) // HEAD_DIM
    ones = (lane_a == lane_b).astype(F32).astype(BF16)

    def head_norm(x, row):
        square = x * x
        high = square.astype(BF16)
        low = (square - high.astype(F32)).astype(BF16)
        mean = (dot(high, ones) + dot(low, ones)) * (1.0 / HEAD_DIM)
        return x * lax.rsqrt(mean + EPS) * qkg[row:row + 1, :]

    def project(p, b, c):
        flat = dot(gath[p, b, c], wq[p])
        queries = (head_norm(flat[:, :aw], 2 * p) * (HEAD_DIM ** -0.5)).astype(BF16)
        key_rows = head_norm(flat[:, aw:2 * aw], 2 * p + 1).astype(BF16)
        return queries, key_rows, flat[:, 2 * aw:].astype(BF16)

    def lanes_of(block):
        return pl.ds(pl.multiple_of(block * aw, aw), aw)

    def att_copy(p, c, source, target):
        return remote_copy(attb.at[p, target, c], att.at[p, c, :, lanes_of(source)],
                           at_s.at[p, c, target], at_r.at[p, c, source], {"ta": target})

    def rs_copy(c):
        return remote_copy(pbuf.at[1, c], prec.at[c], rs_s.at[c], rs_r.at[c], {"ta": partner})

    def total_of(p, c):
        for k in range(1, n_ta):
            source = block_at(k)
            att_copy(p, c, source, source).wait_recv()
        return stream[p // 2, c] + dot(att[p, c], wo[p].reshape(n_ta * aw, model))

    def out_ready(p):
        for slot in range(2):
            far_d(p, slot).wait_recv()

    def pick_rows(source):
        return (source == lax.broadcasted_iota(jnp.int32, (1, piece), 1)).astype(F32).astype(BF16)

    index = lax.broadcasted_iota(jnp.int32, (piece, 1), 0)

    def digits(value, sizes):
        found = []
        for size in sizes[::-1]:
            found.append(lax.rem(value, size))
            value = lax.div(value, size)
        return found[::-1]

    def number(parts, sizes):
        value = parts[0]
        for part, size in zip(parts[1:], sizes[1:]):
            value = value * size + part
        return value

    def x1_copy(c, source, target):
        return remote_copy(sx1.at[c, target], x1.at[c, source], x1_s.at[c, target], x1_r.at[c, source],
                           group_place(target))

    def x1_send(c):
        w, h, f, r, q = digits(index, (n_wa, n_ha, some_frames, sub_rows, sub_cols))
        source = number((w, f, r, h, q), (n_wa, some_frames, sub_rows, n_ha, sub_cols))
        moved = dot(pick_rows(source), total_of(0, c).astype(BF16)).astype(BF16)
        sx1[c] = moved.reshape(groups, unit, model)
        for step in range(1, groups):
            x1_copy(c, here, lax.rem(here + step, groups)).start()
        x1[c, here] = sx1[c, here]

    def x1_take(c):
        for step in range(1, groups):
            source = lax.rem(here + step, groups)
            x1_copy(c, source, source).wait_recv()
        stream[0, c] = x1[c].reshape(piece, model).astype(F32)
        norm_start(1, c)

    def fo_copy(c, source, target):
        return remote_copy(fo.at[c, :, :, target], ro.at[c, source], fo_s.at[c, target], fo_r.at[c, source],
                           {"ha": target})

    def fo_send(c):
        rs_copy(c).wait_recv()
        near = pbuf[0, c].astype(F32) + prec[c].astype(F32)
        total = (stream[1, c] + near).astype(BF16)
        fo[c] = total.reshape(CHUNKS, some_wa, n_ha, unit, model)
        for step in range(1, n_ha):
            fo_copy(c, at_ha, lax.rem(at_ha + step, n_ha)).start()
        ro[c, at_ha] = fo[c, :, :, at_ha]

    def fo_take(c):
        for step in range(1, n_ha):
            source = lax.rem(at_ha + step, n_ha)
            fo_copy(c, source, source).wait_recv()
        f0, f1, w, r, h, q = digits(index, (CHUNKS, some_frames, some_wa, sub_rows, n_ha, sub_cols))
        source = number((h, f0, w, f1, r, q), (n_ha, CHUNKS, some_wa, some_frames, sub_rows, sub_cols))
        moved = dot(pick_rows(source), ro[c].reshape(piece, model)).astype(BF16)
        out[:, c * some_wa:(c + 1) * some_wa] = moved.reshape(frames, some_wa, sub_rows * width, model)

    pl.semaphore_wait(barrier, greets)
    for c in range(CHUNKS):
        for step in range(1, n_wa):
            x0_copy(c, at_wa, lax.rem(at_wa + step, n_wa)).start()
    far_x(0).start()

    def begin(c, part, tokens):
        at = rows_of(part)
        stream[0, c, at] = tokens.reshape(part_rows, model).astype(F32)
        norm_rows(0, c, at)
        ag_part(0, c, part)

    for c in range(CHUNKS):
        begin(c, at_wa, tok[c * some_frames:(c + 1) * some_frames, at_wa])
    for j in range(3):
        far_d(j, 0).start()
    for j in (1, 2):
        far_x(j).start()
    for c in range(CHUNKS):
        for step in range(1, n_wa):
            source = lax.rem(at_wa + step, n_wa)
            x0_copy(c, source, source).wait_recv()
            begin(c, source, x0[c, source])
    far_first(0)
    far_own(0)

    column = lax.broadcasted_iota(jnp.int32, (1, piece), 1)

    def lines_0(at):
        w, f, r, q = digits(at, (n_wa, some_frames, sub_rows, width))
        return f * sub_rows + r

    def lines_1(at):
        g, f, r, q = digits(at, (groups, some_frames, sub_rows, sub_cols))
        return f * sub_cols + q

    def line_step(p, i, mask):
        k, c = arrival(i)
        b = block_at(k)
        ag_wait(p, k, c)
        queries, key_rows, values = project(p, b, c)
        done = attend(queries, key_rows, values, mask)

        @pl.when(k == 0)
        def _():
            att[p, c, :, lanes_of(me)] = done

        @pl.when(k > 0)
        def _():
            attb[p, b, c] = done
            att_copy(p, c, me, b).start()

    def after(i, step, actions):
        @pl.when(i == step)
        def _():
            for action, args in actions:
                action(*args)

    def start_x(j):
        far_x(j).start()

    ready(0)
    mask_0 = lines_0(index) == lines_0(column)

    def pass_0(i, _):
        line_step(0, i, mask_0)
        after(i, 1, [(far_next, (0,)), (far_first, (1,))])
        after(i, 3, [(far_pair, (0,))])
        after(i, 5, [(start_x, (3,))])
        after(i, 7, [(start_x, (4,)), (start_x, (5,))])
        return 0

    lax.fori_loop(0, steps, pass_0, 0)
    ready(1)
    out_ready(0)
    x1_send(0)
    x1_take(0)
    ready(2)
    mask_1 = lines_1(index) == lines_1(column)

    def pass_1(i, _):
        for c in range(1, CHUNKS):
            after(i, 2 * c - 1, [(x1_send, (c,))])
            after(i, 2 * c, [(x1_take, (c,))])
        after(i, 2, [(far_own, (1,)), (far_next, (1,)), (far_first, (2,)), (far_first, (3,))])
        after(i, 3, [(far_own, (2,)), (far_own, (3,)), (far_first, (4,)), (far_first, (5,))])
        after(i, 5, [(far_pair, (1,))])
        line_step(1, i, mask_1)
        return 0

    lax.fori_loop(0, steps, pass_1, 0)
    ready(3)
    out_ready(1)
    far_next(2)
    half_piece = piece // CHUNKS
    for c in range(CHUNKS):
        total = total_of(1, c)
        for d in range(CHUNKS):
            stream[1, d, c * half_piece:(c + 1) * half_piece] = total[d * half_piece:(d + 1) * half_piece]
    for d in range(CHUNKS):
        norm_start(2, d)
    for at in (4, 5):
        ready(at)
    far_next(3)
    for j in (4, 5):
        far_own(j)
    t_i = lax.div(index, unit) * some_frames + lax.div(lax.rem(index, unit), spots)
    t_j = lax.div(column, unit) * some_frames + lax.div(lax.rem(column, unit), spots)
    causal = (lax.rem(index, spots) == lax.rem(column, spots)) & (t_i >= t_j)

    def time_project(i, _):
        k, c = arrival(i)
        b = block_at(k)
        ag_wait(2, k, c)
        queries, key_rows, values = project(2, b, c)
        pk2[c, b, :, :, :, 0:aw] = queries.reshape(CHUNKS, some_groups, unit, aw)
        pk2[c, b, :, :, :, aw:2 * aw] = key_rows.reshape(CHUNKS, some_groups, unit, aw)
        pk2[c, b, :, :, :, 2 * aw:3 * aw] = values.reshape(CHUNKS, some_groups, unit, aw)
        return 0

    def time_attend(i, _):
        c = lax.div(i, some_groups)
        g = lax.rem(i, some_groups)
        done = attend(
            pk2[c, :, :, g, :, 0:aw].reshape(piece, aw),
            pk2[c, :, :, g, :, aw:2 * aw].reshape(piece, aw),
            pk2[c, :, :, g, :, 2 * aw:3 * aw].reshape(piece, aw),
            causal,
        )
        for b in range(n_ta):
            for at in range(CHUNKS):
                start = (b * CHUNKS + at) * unit
                rows = pl.ds(pl.multiple_of((at * some_groups + g) * unit, unit), unit)
                attb[2, b, c, rows] = done[start:start + unit]
        return 0

    lax.fori_loop(0, early, time_project, 0)

    def time_chunk(c, _):
        lax.fori_loop(early + 2 * c, early + 2 * c + 2, time_project, 0)
        lax.fori_loop(c * some_groups, (c + 1) * some_groups, time_attend, 0)
        for k in (2, 3, 1):
            att_copy(2, c, me, block_at(k)).start()
        att[2, c, :, lanes_of(me)] = attb[2, me, c]

        @pl.when(c == 0)
        def _():
            far_pair(2)
            far_next(4)
        return 0

    lax.fori_loop(0, CHUNKS, time_chunk, 0)

    for at in (6, 7):
        ready(at)
    out_ready(2)
    far_next(5)
    half = wf.shape[0]

    def silu_part(x, w_in, w_out):
        both = dot(x, w_in)
        gate, up = both[:, :half], both[:, half:]
        hidden = (gate / (1.0 + jnp.exp(-gate)) * up).astype(BF16)
        return dot(hidden, w_out)

    def mlp(i, _):
        k, c = lax.rem(i, 2), lax.div(i, 2)
        b = block_at(k)

        for d in range(CHUNKS):
            @pl.when(i == 2 * d)
            def _():
                stream[1, d] = total_of(2, d)
                norm_rows(3, d, pl.ds(0, piece))
                for part in range(n_wa):
                    ag_copy(3, 0, d, part).start()
                if d == 0:
                    for j in (3, 4, 5):
                        far_ready(j)

        @pl.when(k == 1)
        def _():
            for part in range(n_wa):
                ag_copy(3, 0, c, part).wait_recv()

        x = gath[3, b, c]
        part = silu_part(x, wi[...], wf[...]) + silu_part(
            x, wi_far[...].reshape(model, 2 * half), wf_far[...].reshape(half, model))
        pbuf[k, c] = part.astype(BF16)

        @pl.when(k == 1)
        def _():
            rs_copy(c).start()

        return 0

    lax.fori_loop(0, 2 * CHUNKS, mlp, 0)
    for c in range(CHUNKS):
        fo_send(c)
    for c in range(CHUNKS):
        fo_take(c)

    for c in range(CHUNKS):
        for step in range(1, n_wa):
            x0_copy(c, at_wa, lax.rem(at_wa + step, n_wa)).wait_send()
        for step in range(1, groups):
            x1_copy(c, here, lax.rem(here + step, groups)).wait_send()
        for step in range(1, n_ha):
            fo_copy(c, at_ha, lax.rem(at_ha + step, n_ha)).wait_send()
        for part in range(n_wa):
            for p in range(3):
                for slot in range(3):
                    ag_copy(p, slot, c, part).wait_send()
            ag_copy(3, 0, c, part).wait_send()
        for p in range(3):
            for k in range(1, n_ta):
                att_copy(p, c, me, block_at(k)).wait_send()
        rs_copy(c).wait_send()
    for j in range(6):
        far_x(j).wait_send()
        for step in range(1, n_ha):
            far_z(j, at_ha, lax.rem(at_ha + step, n_ha)).wait_send()
        for step in range(1, n_wa):
            for part in range(n_ha):
                far_y(j, at_wa, part, lax.rem(at_wa + step, n_wa)).wait_send()
    for j in range(3):
        for slot in range(2):
            far_d(j, slot).wait_send()


def axial_local(sizes, tokens, norm_gain, qkv_weight, qk_gain, out_weight, ffn_in, ffn_out):
    n_ta, n_ha, n_wa = sizes
    extent = tokens.shape
    clips, frames, height, width, model = extent
    frames = clips * frames
    rows = frames * height * width
    piece = rows // CHUNKS
    aw = qkv_weight.shape[-1]
    half = ffn_in.shape[-1]
    groups = n_ha * n_wa
    unit = piece // groups
    sub = height // n_wa * width
    heads = aw // HEAD_DIM
    gains = jnp.tile(qk_gain.reshape(-1, HEAD_DIM), (1, heads))
    dma = pltpu.SemaphoreType.DMA
    vm = pltpu.VMEM
    scratch = [
        vm((CHUNKS, n_wa, frames // CHUNKS, sub, model), BF16),
        vm((2, CHUNKS, piece, model), F32),
        vm((4, n_ta, CHUNKS, piece, model), BF16),
        vm((3, model, 3 * aw), BF16),
        vm((3, n_ta, n_wa, n_ha, aw // groups, model), BF16),
        vm((model, 2 * half), BF16),
        vm((half, model), BF16),
        vm((2, n_wa, n_ha, model // groups // 2, 2 * half), BF16),
        vm((n_wa, n_ha, half // groups, model), BF16),
        vm((CHUNKS, groups, unit, model), BF16),
        vm((CHUNKS, groups, unit, model), BF16),
        vm((CHUNKS, n_ta, CHUNKS, groups // CHUNKS, unit, 3 * aw), BF16),
        vm((3, n_ta, CHUNKS, piece, aw), BF16),
        vm((3, CHUNKS, piece, n_ta * aw), BF16),
        vm((2, CHUNKS, piece, model), BF16),
        vm((CHUNKS, piece, model), BF16),
        vm((CHUNKS, CHUNKS, n_wa // CHUNKS, n_ha, unit, model), BF16),
        vm((CHUNKS, n_ha, CHUNKS, n_wa // CHUNKS, unit, model), BF16),
        dma((4, 4)),
        dma((CHUNKS, n_wa)),
        dma((CHUNKS, n_wa)),
        dma((4, 3, CHUNKS, n_wa)),
        dma((4, 3, CHUNKS, n_wa)),
        dma((CHUNKS,)),
        dma((CHUNKS,)),
        dma((3, CHUNKS, n_ta)),
        dma((3, CHUNKS, n_ta)),
        dma((CHUNKS, groups)),
        dma((CHUNKS, groups)),
        dma((CHUNKS, n_ha)),
        dma((CHUNKS, n_ha)),
        dma((6,)),
        dma((6,)),
        dma((6, n_ha)),
        dma((6, n_ha)),
        dma((6, n_wa, n_ha)),
        dma((6, n_wa, n_ha)),
        dma((3, 2)),
        dma((3, 2)),
    ]
    vmem = pl.BlockSpec(memory_space=pltpu.VMEM)
    anyw = pl.BlockSpec(memory_space=pl.ANY)
    result = pl.pallas_call(
        functools.partial(axial_kernel, (n_ta, n_ha, n_wa, frames, height, width)),
        out_shape=jax.ShapeDtypeStruct((frames, n_wa, sub, model), BF16),
        in_specs=[vmem, vmem, vmem, anyw, anyw, anyw, anyw],
        out_specs=vmem,
        scratch_shapes=scratch,
        compiler_params=pltpu.CompilerParams(
            collective_id=0, has_side_effects=True, vmem_limit_bytes=67043328),
        name="axial_layer",
    )(
        tokens.reshape(frames, n_wa, sub, model),
        norm_gain,
        gains,
        jnp.transpose(qkv_weight, (0, 2, 1, 3)),
        out_weight.reshape(3, n_wa, n_ha, aw // groups, model),
        ffn_in.reshape(model, 2 * half),
        ffn_out,
    )
    return result.reshape(extent)


def local(sizes, tokens, *weights):
    n_ta, n_ha, n_wa = sizes
    clips, frames, height, width, _ = tokens.shape
    fits = n_wa % CHUNKS == 0 and height % n_wa == 0 and width % n_ha == 0 and clips * frames % CHUNKS == 0
    unit = clips * frames * height * width // (CHUNKS * n_ha * n_wa)
    if fits and unit % 16 == 0:
        return axial_local(sizes, tokens, *weights)
    return general_local(sizes, tokens, *weights)


def solution(mesh):
    sizes = tuple(mesh.shape[name] for name in ("ta", "ha", "wa"))
    return jax.shard_map(
        functools.partial(local, sizes),
        mesh=mesh,
        in_specs=(
            P(None, "ta", "ha", "wa", None),
            P(),
            P(None, None, None, "ta"),
            P(),
            P(None, "ta", None),
            P(None, None, "ta"),
            P("ta", None),
        ),
        out_specs=P(None, "ta", "ha", "wa", None),
        check_vma=False,
    )
```

```python
import functools

import jax
import jax.numpy as jnp
from jax import lax
from jax.experimental import pallas as pl
from jax.experimental.pallas import tpu as pltpu
from jax.sharding import PartitionSpec as P

HEAD_DIM = 64
CHUNKS = 2
EPS = 1e-06
MESH = pl.DeviceIdType.MESH
F32 = jnp.float32
BF16 = jnp.bfloat16


def dot(a, b):
    return jnp.dot(a, b, preferred_element_type=F32)


def dot_t(a, b):
    return lax.dot_general(a, b, (((1,), (1,)), ((), ())), preferred_element_type=F32)


def attend(queries, key_rows, values, mask):
    width = queries.shape[-1]
    lane_head = lax.broadcasted_iota(jnp.int32, (1, width), 1) // HEAD_DIM
    total = None
    for head in range(width // HEAD_DIM):
        pick = (lane_head == head).astype(F32).astype(BF16)
        scores = dot_t(queries * pick, key_rows)
        weights = jnp.where(mask, jnp.exp(scores), 0.0)
        probs = weights * (1.0 / jnp.sum(weights, axis=-1, keepdims=True))
        part = dot(probs.astype(BF16), values * pick)
        total = part if total is None else total + part
    return total.astype(BF16)


class Plan:
    def __init__(self, n, n_ta, frames, rows):
        self.n = n
        self.m = frames
        self.unit = rows // frames
        self.low = min(n, frames)
        self.q = frames // self.low
        self.blocks = n_ta * frames // max(n, frames)
        self.u = self.blocks * self.q


def general_kernel(cfg, tok, gain, qkg, wq_h, wo_h, wi_h, wf_h, out, *s):
    n_ta, frames, height, width, plans = cfg
    (stream, gath, wq, wo, wi, wf, pk, a0, a1, res0, res1, att, pk2, att2, pbuf, prec, comb, xrec,
     wsem, ag_s, ag_r, s10, r10, s20, r20, s11, r11, s21, r21, rs_s, rs_r) = s
    rows = tok.shape[0]
    per_frame = height * width
    aw = wo.shape[1]
    me = lax.axis_index("ta")
    core, chip = lax.rem(me, 2), lax.div(me, 2)

    def block_at(k):
        return lax.rem(chip + lax.div(k, 2), 2) * 2 + lax.rem(core + lax.rem(k, 2), 2)

    piece = rows // CHUNKS
    wide = lambda c: pl.ds(pl.multiple_of(c * piece, piece), piece)
    steps = n_ta * CHUNKS
    early = 2 * CHUNKS

    def arrival(i):
        late = i - early
        k = jnp.where(i < early, lax.div(i, CHUNKS), 2 + lax.rem(late, 2))
        c = jnp.where(i < early, lax.rem(i, CHUNKS), lax.div(late, 2))
        return k, c

    def departure(i):
        rest = i - early
        k = jnp.where(i < early, 3 - lax.rem(i, 2), 1 - lax.div(rest, CHUNKS))
        c = jnp.where(i < early, lax.div(i, 2), lax.rem(rest, CHUNKS))
        return k, c

    partner = block_at(1)
    remote = block_at(2)
    pair_last = block_at(3)

    copies = []
    for at in range(3):
        copies.append([
            pltpu.make_async_copy(wq_h.at[at, j], wq.at[at, :, j * aw:(j + 1) * aw], wsem.at[at, j])
            for j in range(3)])
        copies.append([pltpu.make_async_copy(wo_h.at[at], wo.at[at], wsem.at[at, 3])])
    copies.append([pltpu.make_async_copy(wi_h, wi, wsem.at[3, 0])])
    copies.append([pltpu.make_async_copy(wf_h, wf, wsem.at[3, 1])])
    for group in copies:
        for copy in group:
            copy.start()

    def ready(at):
        for copy in copies[at]:
            copy.wait()

    barrier = pltpu.get_barrier_semaphore()
    greets = 0
    for other in (partner, remote):
        pl.semaphore_signal(barrier, inc=1, device_id={"ta": other}, device_id_type=MESH)
        greets += 1
    for axis, plan in plans:
        here = lax.axis_index(axis)
        for step in range(1, plan.n):
            other = lax.rem(here + step, plan.n)
            pl.semaphore_signal(barrier, inc=1, device_id={axis: other}, device_id_type=MESH)
            greets += 1

    def remote_copy(src, dst, send, recv, axis, other):
        return pltpu.make_async_remote_copy(
            src_ref=src, dst_ref=dst, send_sem=send, recv_sem=recv,
            device_id={axis: other}, device_id_type=MESH)

    def norm_own(p, c):
        x = stream[wide(c), :]
        scale = lax.rsqrt(jnp.mean(x * x, axis=-1, keepdims=True) + EPS)
        gath[p, me, wide(c)] = (x * scale * gain[p:p + 1, :]).astype(BF16)

    def ag_copy(p, slot, c):
        block = me if slot < 2 else remote
        other = remote if slot == 1 else partner
        ref = gath.at[p, block, wide(c)]
        return remote_copy(ref, ref, ag_s.at[p, slot, c], ag_r.at[p, slot, c], "ta", other)

    def ag_start(p, c):
        ag_copy(p, 1, c).start()
        ag_copy(p, 0, c).start()

    def ag_wait(p, k, c):
        @pl.when(k == 1)
        def _():
            ag_copy(p, 0, c).wait_recv()

        @pl.when(k == 2)
        def _():
            ag_copy(p, 1, c).wait_recv()
            ag_copy(p, 2, c).start()

        @pl.when(k == 3)
        def _():
            ag_copy(p, 2, c).wait_recv()

    lane_a = lax.broadcasted_iota(jnp.int32, (aw, aw), 0) // HEAD_DIM
    lane_b = lax.broadcasted_iota(jnp.int32, (aw, aw), 1) // HEAD_DIM
    ones = (lane_a == lane_b).astype(F32).astype(BF16)

    def head_norm(x, row):
        square = x * x
        high = square.astype(BF16)
        low = (square - high.astype(F32)).astype(BF16)
        mean = (dot(high, ones) + dot(low, ones)) * (1.0 / HEAD_DIM)
        return x * lax.rsqrt(mean + EPS) * qkg[row:row + 1, :]

    def project(p, b, c):
        flat = dot(gath[p, b, wide(c)], wq[p])
        queries = (head_norm(flat[:, :aw], 2 * p) * (HEAD_DIM ** -0.5)).astype(BF16)
        key_rows = head_norm(flat[:, aw:2 * aw], 2 * p + 1).astype(BF16)
        return queries, key_rows, flat[:, 2 * aw:].astype(BF16)

    def rs_copy(p, slot, c):
        send, recv = rs_s.at[p, slot, c], rs_r.at[p, slot, c]
        if slot == 2:
            return remote_copy(comb.at[p, wide(c)], xrec.at[p, wide(c)], send, recv, "ta", remote)
        return remote_copy(pbuf.at[p, 2 * slot + 1, wide(c)], prec.at[p, slot, wide(c)], send, recv, "ta", partner)

    def rs_put(p, k, c, part):
        pbuf[p, k, wide(c)] = part.astype(BF16)

        @pl.when(k == 1)
        def _():
            rs_copy(p, 0, c).start()

        @pl.when(k == 3)
        def _():
            rs_copy(p, 1, c).start()

    def rs_combine(p, c):
        rs_copy(p, 1, c).wait_recv()
        comb[p, wide(c)] = (pbuf[p, 2, wide(c)].astype(F32) + prec[p, 1, wide(c)].astype(F32)).astype(BF16)
        rs_copy(p, 2, c).start()

    def rs_total(p, c):
        rs_copy(p, 0, c).wait_recv()
        near = pbuf[p, 0, wide(c)].astype(F32) + prec[p, 0, wide(c)].astype(F32)
        rs_copy(p, 2, c).wait_recv()
        return stream[wide(c), :] + (near + xrec[p, wide(c)].astype(F32))

    def turn(p):
        for c in range(CHUNKS):
            stream[wide(c), :] = rs_total(p, c)
            norm_own(p + 1, c)
            ag_start(p + 1, c)

    stream[...] = tok[...].astype(F32)
    norm_own(0, 0)
    pl.semaphore_wait(barrier, greets)
    ag_start(0, 0)
    for c in range(1, CHUNKS):
        norm_own(0, c)
        ag_start(0, c)

    sends = []
    for p in (0, 1):
        axis, plan = plans[p]
        n, m, unit, groups, low, fold, span = plan.n, plan.m, plan.unit, plan.u, plan.low, plan.q, plan.blocks
        here = lax.axis_index(axis)
        abuf, res = ((a0, res0), (a1, res1))[p]
        s1, r1, s2, r2 = ((s10, r10, s20, r20), (s11, r11, s21, r21))[p]
        ready(2 * p)

        def owner_of(b, j, m=m, low=low, span=span):
            return lax.rem(j, low) + m * lax.div(b, span)

        def place(j, unit=unit):
            return pl.ds(pl.multiple_of(j * unit, unit), unit)

        def unit_copy(b, j, p=p, axis=axis, low=low, fold=fold, span=span, here=here, abuf=abuf, s1=s1, r1=r1,
                      owner_of=owner_of, place=place):
            owner = owner_of(b, j)
            u = lax.rem(b, span) * fold + lax.div(j, low)
            return owner, u, remote_copy(
                pk.at[p, b, place(j)], abuf.at[u, here], s1.at[b, j], r1.at[u, here], axis, owner)

        def first(i, _, p=p, m=m, here=here, abuf=abuf, unit_copy=unit_copy, place=place):
            k, c = arrival(i)
            b = block_at(k)
            ag_wait(p, k, c)
            queries, key_rows, values = project(p, b, c)
            pk[p, b, wide(c), 0:aw] = queries
            pk[p, b, wide(c), aw:2 * aw] = key_rows
            pk[p, b, wide(c), 2 * aw:3 * aw] = values
            for at in range(m // CHUNKS):
                j = c * (m // CHUNKS) + at
                owner, u, copy = unit_copy(b, j)

                @pl.when(owner != here)
                def _():
                    copy.start()

                @pl.when(owner == here)
                def _():
                    abuf[u, here] = pk[p, b, place(j), :]
            return 0

        lax.fori_loop(0, steps, first, 0)

        size = n * unit
        if p == 0:
            line_of = lambda at: lax.div(lax.rem(at, unit), width)
        else:
            line_of = lambda at: lax.div(lax.rem(at, unit), per_frame) * width + lax.rem(at, width)
        mask = line_of(lax.broadcasted_iota(jnp.int32, (size, 1), 0)) == line_of(
            lax.broadcasted_iota(jnp.int32, (1, size), 1))

        def home(u, m=m, low=low, fold=fold, span=span, here=here):
            return lax.div(u, fold) + span * lax.div(here, m), lax.rem(here, low) + low * lax.rem(u, fold)

        def back_copy(u, other, p=p, axis=axis, res=res, s2=s2, r2=r2, home=home, place=place):
            b, j = home(u)
            return remote_copy(
                res.at[u, other], att.at[p, b, place(j)], s2.at[u, other], r2.at[b, j], axis, other)

        def second(i, _, p=p, axis=axis, n=n, unit=unit, fold=fold, span=span, here=here, abuf=abuf, res=res,
                   r1=r1, s1=s1, mask=mask, size=size, back_copy=back_copy, home=home, place=place):
            k, sub = arrival(i) if fold == CHUNKS else (lax.div(i, fold), lax.rem(i, fold))
            u = lax.rem(block_at(k), span) * fold + sub
            for step in range(1, n):
                source = lax.rem(here + step, n)
                remote_copy(abuf.at[u, source], abuf.at[u, source], s1.at[0, 0], r1.at[u, source],
                            axis, source).wait_recv()
            done = attend(
                abuf[u, :, :, 0:aw].reshape(size, aw),
                abuf[u, :, :, aw:2 * aw].reshape(size, aw),
                abuf[u, :, :, 2 * aw:3 * aw].reshape(size, aw),
                mask,
            )
            res[u] = done.reshape(n, unit, aw)
            for step in range(1, n):
                back_copy(u, lax.rem(here + step, n)).start()
            b, j = home(u)
            att[p, b, place(j)] = res[u, here]
            return 0

        lax.fori_loop(0, groups, second, 0)
        ready(2 * p + 1)

        def third(i, _, p=p, axis=axis, m=m, here=here, s2=s2, r2=r2, owner_of=owner_of, place=place):
            k, c = departure(i)
            b = block_at(k)
            for at in range(m // CHUNKS):
                j = c * (m // CHUNKS) + at
                owner = owner_of(b, j)

                @pl.when(owner != here)
                def _():
                    ref = att.at[p, b, place(j)]
                    remote_copy(ref, ref, s2.at[0, 0], r2.at[b, j], axis, owner).wait_recv()
            rs_put(p, k, c, dot(att[p, b, wide(c)], wo[p]))

            @pl.when(k == 2)
            def _():
                rs_combine(p, c)
            return 0

        lax.fori_loop(0, steps, third, 0)
        turn(p)

        def drain(unit_copy=unit_copy, back_copy=back_copy, n=n, m=m, groups=groups, here=here):
            for b in range(n_ta):
                for j in range(m):
                    owner, _, copy = unit_copy(b, j)

                    @pl.when(owner != here)
                    def _():
                        copy.wait_send()
            for u in range(groups):
                for step in range(1, n):
                    back_copy(u, lax.rem(here + step, n)).wait_send()

        sends.append(drain)

    p = 2
    some_frames = frames // CHUNKS
    ready(2 * p)

    def time_first(i, _):
        k, c = arrival(i)
        b = block_at(k)
        ag_wait(p, k, c)
        queries, key_rows, values = project(p, b, c)
        at = pl.ds(b * frames + c * some_frames, some_frames)
        pk2[at, :, 0:aw] = queries.reshape(some_frames, per_frame, aw)
        pk2[at, :, aw:2 * aw] = key_rows.reshape(some_frames, per_frame, aw)
        pk2[at, :, 2 * aw:3 * aw] = values.reshape(some_frames, per_frame, aw)
        return 0

    lax.fori_loop(0, steps, time_first, 0)
    every = n_ta * frames
    some = 16
    size = every * some
    i_at = lax.broadcasted_iota(jnp.int32, (size, 1), 0)
    j_at = lax.broadcasted_iota(jnp.int32, (1, size), 1)
    causal = (lax.rem(i_at, some) == lax.rem(j_at, some)) & (lax.div(i_at, some) >= lax.div(j_at, some))

    def time_second(g, _):
        at = pl.ds(pl.multiple_of(g * some, some), some)
        done = attend(
            pk2[:, at, 0:aw].reshape(size, aw),
            pk2[:, at, aw:2 * aw].reshape(size, aw),
            pk2[:, at, 2 * aw:3 * aw].reshape(size, aw),
            causal,
        )
        att2[:, at, :] = done.reshape(every, some, aw)
        return 0

    lax.fori_loop(0, per_frame // some, time_second, 0)
    ready(2 * p + 1)

    def time_third(i, _):
        k, c = departure(i)
        b = block_at(k)
        at = pl.ds(b * frames + c * some_frames, some_frames)
        rs_put(p, k, c, dot(att2[at].reshape(piece, aw), wo[p]))

        @pl.when(k == 2)
        def _():
            rs_combine(p, c)
        return 0

    lax.fori_loop(0, steps, time_third, 0)
    turn(p)

    ready(6)
    ready(7)
    half = wf.shape[0]

    def mlp(i, _):
        k, c = arrival(i)
        b = block_at(k)
        ag_wait(3, k, c)
        both = dot(gath[3, b, wide(c)], wi[...])
        gate, up = both[:, :half], both[:, half:]
        hidden = (gate / (1.0 + jnp.exp(-gate)) * up).astype(BF16)
        rs_put(3, k, c, dot(hidden, wf[...]))

        @pl.when((k == 2) & (c > 0))
        def _():
            rs_combine(3, c - 1)
        return 0

    lax.fori_loop(0, steps, mlp, 0)
    rs_combine(3, CHUNKS - 1)
    for c in range(CHUNKS):
        out[wide(c), :] = rs_total(3, c).astype(BF16)

    for drain in sends:
        drain()
    for p in range(4):
        for slot in range(3):
            for c in range(CHUNKS):
                ag_copy(p, slot, c).wait_send()
                rs_copy(p, slot, c).wait_send()


def general_local(sizes, tokens, norm_gain, qkv_weight, qk_gain, out_weight, ffn_in, ffn_out):
    n_ta, n_ha, n_wa = sizes
    extent = tokens.shape
    clips, frames, height, width, model = extent
    rows = clips * frames * height * width
    aw = qkv_weight.shape[-1]
    half = ffn_in.shape[-1]
    plans = (("wa", Plan(n_wa, n_ta, frames, rows)), ("ha", Plan(n_ha, n_ta, frames, rows)))
    cfg = (n_ta, frames, height, width, plans)
    heads = aw // HEAD_DIM
    gains = jnp.tile(qk_gain.reshape(-1, HEAD_DIM), (1, heads))
    dma = pltpu.SemaphoreType.DMA
    vm = pltpu.VMEM
    scratch = [
        vm((rows, model), F32),
        vm((4, n_ta, rows, model), BF16),
        vm((3, model, 3 * aw), BF16),
        vm((3, aw, model), BF16),
        vm((model, 2 * half), BF16),
        vm((half, model), BF16),
        vm((2, n_ta, rows, 3 * aw), BF16),
    ]
    for width_of in (3 * aw, aw):
        for _, plan in plans:
            scratch.append(vm((plan.u, plan.n, plan.unit, width_of), BF16))
    scratch += [
        vm((2, n_ta, rows, aw), BF16),
        vm((n_ta * frames, height * width, 3 * aw), BF16),
        vm((n_ta * frames, height * width, aw), BF16),
        vm((4, n_ta, rows, model), BF16),
        vm((4, 2, rows, model), BF16),
        vm((4, rows, model), BF16),
        vm((4, rows, model), BF16),
        dma((4, 4)),
        dma((4, 3, CHUNKS)),
        dma((4, 3, CHUNKS)),
    ]
    for _, plan in plans:
        scratch += [
            dma((n_ta, plan.m)),
            dma((plan.u, plan.n)),
            dma((plan.u, plan.n)),
            dma((n_ta, plan.m)),
        ]
    scratch += [dma((4, 3, CHUNKS)), dma((4, 3, CHUNKS))]
    vmem = pl.BlockSpec(memory_space=pltpu.VMEM)
    anyw = pl.BlockSpec(memory_space=pl.ANY)
    result = pl.pallas_call(
        functools.partial(general_kernel, cfg),
        out_shape=jax.ShapeDtypeStruct((rows, model), BF16),
        in_specs=[vmem, vmem, vmem, anyw, anyw, anyw, anyw],
        out_specs=vmem,
        scratch_shapes=scratch,
        compiler_params=pltpu.CompilerParams(
            collective_id=0, has_side_effects=True, vmem_limit_bytes=67043328),
        name="axial_layer",
    )(
        tokens.reshape(rows, model),
        norm_gain,
        gains,
        jnp.transpose(qkv_weight, (0, 2, 1, 3)),
        out_weight,
        ffn_in.reshape(model, 2 * half),
        ffn_out,
    )
    return result.reshape(extent)


def axial_kernel(cfg, tok, gain, qkg, wq_h, wo_h, wi_h, wf_h, out, *s):
    n_ta, n_ha, n_wa, frames, height, width = cfg
    (gains, x0, stream, gath, wq, wo, wi, wf, wi_far, wf_far, sx1, x1, pk2, attb, att, pbuf, prec, fo, ro,
     raw_in, wsem, x0_s, x0_r, ag_s, ag_r, rs_s, rs_r, at_s, at_r, x1_s, x1_r, fo_s, fo_r,
     wx_s, wx_r, wz_s, wz_r, wy_s, wy_r, wd_s, wd_r) = s
    model = tok.shape[-1]
    aw = pk2.shape[-1] // 3
    piece = frames * height * width // CHUNKS
    some_frames = frames // CHUNKS
    sub_rows = height // n_wa
    sub_cols = width // n_ha
    spots = sub_rows * sub_cols
    unit = some_frames * spots
    groups = n_ha * n_wa
    some_groups = groups // CHUNKS
    some_wa = n_wa // CHUNKS
    me = lax.axis_index("ta")
    at_ha = lax.axis_index("ha")
    at_wa = lax.axis_index("wa")
    here = at_wa * n_ha + at_ha
    core, chip = lax.rem(me, 2), lax.div(me, 2)

    def block_at(k):
        return lax.rem(chip + lax.div(k, 2), 2) * 2 + lax.rem(core + lax.rem(k, 2), 2)

    partner = block_at(1)
    remote = block_at(2)
    part_rows = piece // n_wa
    steps = n_ta * CHUNKS
    early = 2 * CHUNKS

    def arrival(i):
        late = i - early
        c = jnp.where(i < early, lax.div(i, 2), lax.div(late, 2))
        k = jnp.where(i < early, lax.rem(i, 2), 2 + lax.rem(late, 2))
        return k, c

    copies = []
    for at in range(3):
        copies.append([
            pltpu.make_async_copy(wq_h.at[at, j], wq.at[at, :, j * aw:(j + 1) * aw], wsem.at[at, j])
            for j in range(3)])
        copies.append([pltpu.make_async_copy(wo_h.at[at], wo.at[at, me], wsem.at[at, 3])])
    copies.append([pltpu.make_async_copy(wi_h, raw_in, wsem.at[3, 0])])
    copies.append([pltpu.make_async_copy(wf_h, wf, wsem.at[3, 1])])

    def ready(at):
        for copy in copies[at]:
            copy.wait()

    barrier = pltpu.get_barrier_semaphore()
    for other in (partner, remote):
        pl.semaphore_signal(barrier, inc=1, device_id={"ta": other}, device_id_type=MESH)

    def group_place(g):
        return {"wa": lax.div(g, n_ha), "ha": lax.rem(g, n_ha)}

    for step in range(1, groups):
        pl.semaphore_signal(barrier, inc=1, device_id=group_place(lax.rem(here + step, groups)), device_id_type=MESH)
    greets = groups + 1

    def remote_copy(src, dst, send, recv, place):
        return pltpu.make_async_remote_copy(
            src_ref=src, dst_ref=dst, send_sem=send, recv_sem=recv,
            device_id=place, device_id_type=MESH)

    for at in (6, 0, 1, 2, 3, 4, 5, 7):
        for copy in copies[at]:
            copy.start()

    def x0_copy(c, source, target):
        at = pl.ds(c * some_frames, some_frames)
        return remote_copy(tok.at[at, target], x0.at[c, source], x0_s.at[c, target], x0_r.at[c, source],
                           {"wa": target})

    flat_rows = model // 16

    def flatten(i, _):
        at = pl.ds(pl.multiple_of(i * flat_rows, flat_rows), flat_rows)
        wi[at] = raw_in[at].reshape(flat_rows, wi.shape[1])
        return 0

    parts_half = wf_h.shape[0] // n_wa
    parts_in = model // wi_far.shape[0]

    def far(j, shard):
        if j < 3:
            return wo.at[j, shard]
        return wi_far.at[j - 3]

    def far_x(j):
        dst = far(j, me).at[at_wa, at_ha]
        if j < 3:
            src = wo_h.at[j, at_wa, at_ha]
        else:
            size = dst.shape[0]
            first = (j - 3) * parts_in
            src = wi.at[pl.ds(pl.multiple_of(first + here * size, size), size)]
        return remote_copy(src, dst, wx_s.at[j], wx_r.at[j], {"ta": remote})

    def half_x(part):
        size = parts_half // n_ha
        src = wf_h.at[pl.ds(pl.multiple_of(at_wa * parts_half + part * size, size), size)]
        return remote_copy(src, wf_far.at[at_wa, part], wz_s.at[5, part], wz_r.at[5, part], {"ta": remote})

    def half_y(part, source, target):
        ref = wf_far.at[source, part]
        return remote_copy(ref, ref, wy_s.at[5, target, part], wy_r.at[5, source, part], {"wa": target})

    def half_start(first, last):
        for part in range(first, last):
            half_x(part).start()

    def half_next(first, last):
        for part in range(first, last):
            half_x(part).wait_recv()
            for step in range(1, n_wa):
                half_y(part, at_wa, lax.rem(at_wa + step, n_wa)).start()

    def half_ready():
        for step in range(1, n_wa):
            source = lax.rem(at_wa + step, n_wa)
            for part in range(n_ha):
                half_y(part, source, source).wait_recv()

    def far_z(j, source, target):
        ref = far(j, remote).at[at_wa, source]
        return remote_copy(ref, ref, wz_s.at[j, target], wz_r.at[j, source], {"ha": target})

    def far_y(j, wa_source, part, target):
        ref = far(j, remote).at[wa_source, part]
        return remote_copy(ref, ref, wy_s.at[j, target, part], wy_r.at[j, wa_source, part], {"wa": target})

    def far_d(j, slot):
        if slot == 0:
            return remote_copy(wo_h.at[j], wo.at[j, me], wd_s.at[j, 0], wd_r.at[j, 0], {"ta": partner})
        ref = wo.at[j, remote]
        return remote_copy(ref, ref, wd_s.at[j, 1], wd_r.at[j, 1], {"ta": partner})

    def far_spread(j, part):
        for step in range(1, n_wa):
            far_y(j, at_wa, part, lax.rem(at_wa + step, n_wa)).start()

    def far_first(j):
        far_x(j).wait_recv()
        for step in range(1, n_ha):
            far_z(j, at_ha, lax.rem(at_ha + step, n_ha)).start()

    def far_own(j):
        far_spread(j, at_ha)

    def far_next(j, first, last):
        for step in range(first, last):
            source = lax.rem(at_ha + step, n_ha)
            far_z(j, source, source).wait_recv()
            far_spread(j, source)

    def far_ready(j):
        for step in range(1, n_wa):
            source = lax.rem(at_wa + step, n_wa)
            for part in range(n_ha):
                far_y(j, source, part, source).wait_recv()

    def far_pair(j):
        far_ready(j)
        far_d(j, 1).start()

    def norm_rows(p, c, at):
        x = stream[p // 2, c, at]
        scale = lax.rsqrt(jnp.mean(x * x, axis=-1, keepdims=True) + EPS)
        gath[p, me, c, at] = (x * scale * gain[p:p + 1, :]).astype(BF16)

    def rows_of(part):
        start = part * part_rows
        return pl.ds(start if isinstance(part, int) else pl.multiple_of(start, part_rows), part_rows)

    def ag_copy(p, slot, c, part):
        block = me if slot < 2 else remote
        other = remote if slot == 1 else partner
        ref = gath.at[p, block, c, rows_of(part)]
        return remote_copy(ref, ref, ag_s.at[p, slot, c, part], ag_r.at[p, slot, c, part], {"ta": other})

    def ag_part(p, c, part):
        ag_copy(p, 1, c, part).start()
        ag_copy(p, 0, c, part).start()

    def norm_start(p, c):
        norm_rows(p, c, pl.ds(0, piece))
        for part in range(n_wa):
            ag_part(p, c, part)

    def ag_wait(p, k, c):
        @pl.when(k == 1)
        def _():
            for part in range(n_wa):
                ag_copy(p, 0, c, part).wait_recv()

        @pl.when(k == 2)
        def _():
            for part in range(n_wa):
                ag_copy(p, 1, c, part).wait_recv()
                ag_copy(p, 2, c, part).start()

        @pl.when(k == 3)
        def _():
            for part in range(n_wa):
                ag_copy(p, 2, c, part).wait_recv()

    lane_a = lax.broadcasted_iota(jnp.int32, (aw, aw), 0) // HEAD_DIM
    lane_b = lax.broadcasted_iota(jnp.int32, (aw, aw), 1) // HEAD_DIM
    ones = (lane_a == lane_b).astype(F32).astype(BF16)

    for p in range(3):
        gains[2 * p:2 * p + 2, :] = jnp.concatenate([qkg[p]] * (aw // HEAD_DIM), axis=1)

    def head_norm(x, row):
        square = x * x
        mean = dot(square.astype(BF16), ones) * (1.0 / HEAD_DIM)
        return x * lax.rsqrt(mean + EPS) * gains[row:row + 1, :]

    def project(p, b, c):
        flat = dot(gath[p, b, c], wq[p])
        queries = (head_norm(flat[:, :aw], 2 * p) * (HEAD_DIM ** -0.5)).astype(BF16)
        key_rows = head_norm(flat[:, aw:2 * aw], 2 * p + 1).astype(BF16)
        return queries, key_rows, flat[:, 2 * aw:].astype(BF16)

    def lanes_of(block):
        return pl.ds(pl.multiple_of(block * aw, aw), aw)

    def att_copy(p, c, source, target):
        return remote_copy(attb.at[p, target, c], att.at[p, c, :, lanes_of(source)],
                           at_s.at[p, c, target], at_r.at[p, c, source], {"ta": target})

    def rs_copy(c):
        return remote_copy(pbuf.at[1, c], prec.at[c], rs_s.at[c], rs_r.at[c], {"ta": partner})

    def total_of(p, c):
        for k in range(1, n_ta):
            source = block_at(k)
            att_copy(p, c, source, source).wait_recv()
        return stream[p // 2, c] + dot(att[p, c], wo[p].reshape(n_ta * aw, model))

    def out_ready(p):
        for slot in range(2):
            far_d(p, slot).wait_recv()

    def pick_rows(source):
        return (source == lax.broadcasted_iota(jnp.int32, (1, piece), 1)).astype(F32).astype(BF16)

    index = lax.broadcasted_iota(jnp.int32, (piece, 1), 0)

    def digits(value, sizes):
        found = []
        for size in sizes[::-1]:
            found.append(lax.rem(value, size))
            value = lax.div(value, size)
        return found[::-1]

    def number(parts, sizes):
        value = parts[0]
        for part, size in zip(parts[1:], sizes[1:]):
            value = value * size + part
        return value

    def x1_copy(c, source, target):
        return remote_copy(sx1.at[c, target], x1.at[c, source], x1_s.at[c, target], x1_r.at[c, source],
                           group_place(target))

    def x1_send(c):
        w, h, f, r, q = digits(index, (n_wa, n_ha, some_frames, sub_rows, sub_cols))
        source = number((w, f, r, h, q), (n_wa, some_frames, sub_rows, n_ha, sub_cols))
        moved = dot(pick_rows(source), total_of(0, c).astype(BF16)).astype(BF16)
        sx1[c] = moved.reshape(groups, unit, model)
        for step in range(1, groups):
            x1_copy(c, here, lax.rem(here + step, groups)).start()
        x1[c, here] = sx1[c, here]

    def x1_take(c):
        for step in range(1, groups):
            source = lax.rem(here + step, groups)
            x1_copy(c, source, source).wait_recv()
        stream[0, c] = x1[c].reshape(piece, model).astype(F32)
        norm_start(1, c)

    def fo_copy(c, source, target):
        return remote_copy(fo.at[c, :, :, target], ro.at[c, source], fo_s.at[c, target], fo_r.at[c, source],
                           {"ha": target})

    def fo_send(c):
        rs_copy(c).wait_recv()
        near = pbuf[0, c].astype(F32) + prec[c].astype(F32)
        total = (stream[1, c] + near).astype(BF16)
        fo[c] = total.reshape(CHUNKS, some_wa, n_ha, unit, model)
        for step in range(1, n_ha):
            fo_copy(c, at_ha, lax.rem(at_ha + step, n_ha)).start()
        ro[c, at_ha] = fo[c, :, :, at_ha]

    def fo_take(c):
        for step in range(1, n_ha):
            source = lax.rem(at_ha + step, n_ha)
            fo_copy(c, source, source).wait_recv()
        f0, f1, w, r, h, q = digits(index, (CHUNKS, some_frames, some_wa, sub_rows, n_ha, sub_cols))
        source = number((h, f0, w, f1, r, q), (n_ha, CHUNKS, some_wa, some_frames, sub_rows, sub_cols))
        moved = dot(pick_rows(source), ro[c].reshape(piece, model)).astype(BF16)
        out[:, c * some_wa:(c + 1) * some_wa] = moved.reshape(frames, some_wa, sub_rows * width, model)

    pl.semaphore_wait(barrier, greets)
    for c in range(CHUNKS):
        for step in range(1, n_wa):
            x0_copy(c, at_wa, lax.rem(at_wa + step, n_wa)).start()
    for j in (0, 1):
        far_x(j).start()

    def begin(c, part, tokens):
        at = rows_of(part)
        stream[0, c, at] = tokens.reshape(part_rows, model).astype(F32)
        norm_rows(0, c, at)
        ag_part(0, c, part)

    for c in range(CHUNKS):
        begin(c, at_wa, tok[c * some_frames:(c + 1) * some_frames, at_wa])
    for j in range(3):
        far_d(j, 0).start()
    ready(6)
    lax.fori_loop(0, model // flat_rows, flatten, 0)
    far_x(3).start()
    for c in range(CHUNKS):
        for step in range(1, n_wa):
            source = lax.rem(at_wa + step, n_wa)
            x0_copy(c, source, source).wait_recv()
            begin(c, source, x0[c, source])
    far_first(0)
    far_own(0)

    column = lax.broadcasted_iota(jnp.int32, (1, piece), 1)

    def lines_0(at):
        w, f, r, q = digits(at, (n_wa, some_frames, sub_rows, width))
        return f * sub_rows + r

    def lines_1(at):
        g, f, r, q = digits(at, (groups, some_frames, sub_rows, sub_cols))
        return f * sub_cols + q

    def line_step(p, i, mask):
        k, c = arrival(i)
        b = block_at(k)
        ag_wait(p, k, c)
        queries, key_rows, values = project(p, b, c)
        done = attend(queries, key_rows, values, mask)

        @pl.when(k == 0)
        def _():
            att[p, c, :, lanes_of(me)] = done

        @pl.when(k > 0)
        def _():
            attb[p, b, c] = done
            att_copy(p, c, me, b).start()

    def after(i, step, actions):
        @pl.when(i == step)
        def _():
            for action, args in actions:
                action(*args)

    def start_x(j):
        far_x(j).start()

    quarter = n_ha // 2
    ready(0)
    mask_0 = lines_0(index) == lines_0(column)

    def pass_0(i, _):
        line_step(0, i, mask_0)
        after(i, 1, [(far_first, (1,)), (far_own, (1,))])
        after(i, 3, [(far_first, (3,)), (far_own, (3,))])
        after(i, 5, [(far_next, (0, 1, n_ha))])
        after(i, 7, [(far_pair, (0,))])
        return 0

    lax.fori_loop(0, steps, pass_0, 0)
    for j in (2, 4):
        far_x(j).start()
    half_start(0, quarter)
    ready(1)
    out_ready(0)
    for c in range(CHUNKS):
        x1_send(c)
    far_next(1, 1, n_ha)
    far_next(3, 1, n_ha)
    x1_take(0)
    ready(2)
    mask_1 = lines_1(index) == lines_1(column)

    def pass_1(i, _):
        for c in range(1, CHUNKS):
            after(i, 2 * c, [(x1_take, (c,))])
        after(i, 2, [(send, (j,)) for j in (2, 4) for send in (far_first, far_own)])
        after(i, 2, [(half_start, (quarter, n_ha)), (half_next, (0, quarter))])
        after(i, 4, [(far_pair, (1,))])
        line_step(1, i, mask_1)
        return 0

    lax.fori_loop(0, steps, pass_1, 0)
    far_next(2, 1, n_ha)
    half_next(quarter, n_ha)
    ready(3)
    out_ready(1)
    half_piece = piece // CHUNKS
    for c in range(CHUNKS):
        total = total_of(1, c)
        for d in range(CHUNKS):
            stream[1, d, c * half_piece:(c + 1) * half_piece] = total[d * half_piece:(d + 1) * half_piece]
    for d in range(CHUNKS):
        norm_start(2, d)
    for at in (4, 5):
        ready(at)
    t_i = lax.div(index, unit) * some_frames + lax.div(lax.rem(index, unit), spots)
    t_j = lax.div(column, unit) * some_frames + lax.div(lax.rem(column, unit), spots)
    causal = (lax.rem(index, spots) == lax.rem(column, spots)) & (t_i >= t_j)

    def time_project(i, _):
        k, c = arrival(i)
        b = block_at(k)
        ag_wait(2, k, c)
        queries, key_rows, values = project(2, b, c)
        pk2[c, b, :, :, :, 0:aw] = queries.reshape(CHUNKS, some_groups, unit, aw)
        pk2[c, b, :, :, :, aw:2 * aw] = key_rows.reshape(CHUNKS, some_groups, unit, aw)
        pk2[c, b, :, :, :, 2 * aw:3 * aw] = values.reshape(CHUNKS, some_groups, unit, aw)
        return 0

    def time_attend(i, _):
        c = lax.div(i, some_groups)
        g = lax.rem(i, some_groups)
        done = attend(
            pk2[c, :, :, g, :, 0:aw].reshape(piece, aw),
            pk2[c, :, :, g, :, aw:2 * aw].reshape(piece, aw),
            pk2[c, :, :, g, :, 2 * aw:3 * aw].reshape(piece, aw),
            causal,
        )
        for b in range(n_ta):
            for at in range(CHUNKS):
                start = (b * CHUNKS + at) * unit
                rows = pl.ds(pl.multiple_of((at * some_groups + g) * unit, unit), unit)
                attb[2, b, c, rows] = done[start:start + unit]
        return 0

    lax.fori_loop(0, early, time_project, 0)
    far_next(4, 1, n_ha)

    def time_chunk(c, _):
        lax.fori_loop(early + 2 * c, early + 2 * c + 2, time_project, 0)
        lax.fori_loop(c * some_groups, (c + 1) * some_groups, time_attend, 0)
        for k in (2, 3, 1):
            att_copy(2, c, me, block_at(k)).start()
        att[2, c, :, lanes_of(me)] = attb[2, me, c]

        @pl.when(c == 0)
        def _():
            far_pair(2)

        return 0

    lax.fori_loop(0, CHUNKS, time_chunk, 0)

    ready(7)
    out_ready(2)
    half = wf.shape[0]

    def silu_part(x, w_in, w_out):
        both = dot(x, w_in)
        gate, up = both[:, :half], both[:, half:]
        hidden = (gate / (1.0 + jnp.exp(-gate)) * up).astype(BF16)
        return dot(hidden, w_out)

    def mlp(i, _):
        k, c = lax.rem(i, 2), lax.div(i, 2)
        b = block_at(k)

        for d in range(CHUNKS):
            @pl.when(i == 2 * d)
            def _():
                if d > 0:
                    fo_send(d - 1)
                stream[1, d] = total_of(2, d)
                norm_rows(3, d, pl.ds(0, piece))
                for part in range(n_wa):
                    ag_copy(3, 0, d, part).start()

        @pl.when(k == 1)
        def _():
            for part in range(n_wa):
                ag_copy(3, 0, c, part).wait_recv()

        x = gath[3, b, c]
        part = silu_part(x, wi[...], wf[...])

        @pl.when(i == 0)
        def _():
            for j in (3, 4):
                far_ready(j)
            half_ready()

        part += silu_part(x, wi_far[...].reshape(model, 2 * half), wf_far[...].reshape(half, model))
        pbuf[k, c] = part.astype(BF16)

        @pl.when(k == 1)
        def _():
            rs_copy(c).start()

        return 0

    lax.fori_loop(0, 2 * CHUNKS, mlp, 0)
    fo_send(CHUNKS - 1)
    for c in range(CHUNKS):
        fo_take(c)

    for c in range(CHUNKS):
        for step in range(1, n_wa):
            x0_copy(c, at_wa, lax.rem(at_wa + step, n_wa)).wait_send()
        for step in range(1, groups):
            x1_copy(c, here, lax.rem(here + step, groups)).wait_send()
        for step in range(1, n_ha):
            fo_copy(c, at_ha, lax.rem(at_ha + step, n_ha)).wait_send()
        for part in range(n_wa):
            for p in range(3):
                for slot in range(3):
                    ag_copy(p, slot, c, part).wait_send()
            ag_copy(3, 0, c, part).wait_send()
        for p in range(3):
            for k in range(1, n_ta):
                att_copy(p, c, me, block_at(k)).wait_send()
        rs_copy(c).wait_send()
    for part in range(n_ha):
        half_x(part).wait_send()
        for step in range(1, n_wa):
            half_y(part, at_wa, lax.rem(at_wa + step, n_wa)).wait_send()
    for j in range(5):
        far_x(j).wait_send()
        for step in range(1, n_ha):
            far_z(j, at_ha, lax.rem(at_ha + step, n_ha)).wait_send()
        for step in range(1, n_wa):
            for part in range(n_ha):
                far_y(j, at_wa, part, lax.rem(at_wa + step, n_wa)).wait_send()
    for j in range(3):
        for slot in range(2):
            far_d(j, slot).wait_send()


def axial_local(sizes, tokens, norm_gain, qkv_weight, qk_gain, out_weight, ffn_in, ffn_out):
    n_ta, n_ha, n_wa = sizes
    extent = tokens.shape
    clips, frames, height, width, model = extent
    frames = clips * frames
    rows = frames * height * width
    piece = rows // CHUNKS
    aw = qkv_weight.shape[-1]
    half = ffn_in.shape[-1]
    groups = n_ha * n_wa
    unit = piece // groups
    sub = height // n_wa * width
    dma = pltpu.SemaphoreType.DMA
    vm = pltpu.VMEM
    scratch = [
        vm((6, aw), F32),
        vm((CHUNKS, n_wa, frames // CHUNKS, sub, model), BF16),
        vm((2, CHUNKS, piece, model), F32),
        vm((4, n_ta, CHUNKS, piece, model), BF16),
        vm((3, model, 3 * aw), BF16),
        vm((3, n_ta, n_wa, n_ha, aw // groups, model), BF16),
        vm((model, 2 * half), BF16),
        vm((half, model), BF16),
        vm((2, n_wa, n_ha, model // groups // 2, 2 * half), BF16),
        vm((n_wa, n_ha, half // groups, model), BF16),
        vm((CHUNKS, groups, unit, model), BF16),
        vm((CHUNKS, groups, unit, model), BF16),
        vm((CHUNKS, n_ta, CHUNKS, groups // CHUNKS, unit, 3 * aw), BF16),
        vm((3, n_ta, CHUNKS, piece, aw), BF16),
        vm((3, CHUNKS, piece, n_ta * aw), BF16),
        vm((2, CHUNKS, piece, model), BF16),
        vm((CHUNKS, piece, model), BF16),
        vm((CHUNKS, CHUNKS, n_wa // CHUNKS, n_ha, unit, model), BF16),
        vm((CHUNKS, n_ha, CHUNKS, n_wa // CHUNKS, unit, model), BF16),
        vm((model, 2, half), BF16),
        dma((4, 4)),
        dma((CHUNKS, n_wa)),
        dma((CHUNKS, n_wa)),
        dma((4, 3, CHUNKS, n_wa)),
        dma((4, 3, CHUNKS, n_wa)),
        dma((CHUNKS,)),
        dma((CHUNKS,)),
        dma((3, CHUNKS, n_ta)),
        dma((3, CHUNKS, n_ta)),
        dma((CHUNKS, groups)),
        dma((CHUNKS, groups)),
        dma((CHUNKS, n_ha)),
        dma((CHUNKS, n_ha)),
        dma((6,)),
        dma((6,)),
        dma((6, n_ha)),
        dma((6, n_ha)),
        dma((6, n_wa, n_ha)),
        dma((6, n_wa, n_ha)),
        dma((3, 2)),
        dma((3, 2)),
    ]
    vmem = pl.BlockSpec(memory_space=pltpu.VMEM)
    anyw = pl.BlockSpec(memory_space=pl.ANY)
    result = pl.pallas_call(
        functools.partial(axial_kernel, (n_ta, n_ha, n_wa, frames, height, width)),
        out_shape=jax.ShapeDtypeStruct((frames, n_wa, sub, model), BF16),
        in_specs=[vmem, vmem, vmem, anyw, anyw, anyw, anyw],
        out_specs=vmem,
        scratch_shapes=scratch,
        compiler_params=pltpu.CompilerParams(
            collective_id=0, has_side_effects=True, vmem_limit_bytes=67043328),
        name="axial_layer",
    )(
        tokens.reshape(frames, n_wa, sub, model),
        norm_gain,
        qk_gain,
        jnp.transpose(qkv_weight, (0, 2, 1, 3)),
        out_weight.reshape(3, n_wa, n_ha, aw // groups, model),
        ffn_in,
        ffn_out,
    )
    return result.reshape(extent)


def local(sizes, tokens, *weights):
    n_ta, n_ha, n_wa = sizes
    clips, frames, height, width, _ = tokens.shape
    fits = n_wa % CHUNKS == 0 and height % n_wa == 0 and width % n_ha == 0 and clips * frames % CHUNKS == 0
    unit = clips * frames * height * width // (CHUNKS * n_ha * n_wa)
    if fits and unit % 16 == 0:
        return axial_local(sizes, tokens, *weights)
    return general_local(sizes, tokens, *weights)


def solution(mesh):
    sizes = tuple(mesh.shape[name] for name in ("ta", "ha", "wa"))
    return jax.shard_map(
        functools.partial(local, sizes),
        mesh=mesh,
        in_specs=(
            P(None, "ta", "ha", "wa", None),
            P(),
            P(None, None, None, "ta"),
            P(),
            P(None, "ta", None),
            P(None, None, "ta"),
            P("ta", None),
        ),
        out_specs=P(None, "ta", "ha", "wa", None),
        check_vma=False,
    )
```

```python
import functools

import jax
import jax.numpy as jnp
from jax import lax
from jax.experimental import pallas as pl
from jax.experimental.pallas import tpu as pltpu
from jax.sharding import PartitionSpec as P

HEAD_DIM = 64
CHUNKS = 2
EPS = 1e-06
MESH = pl.DeviceIdType.MESH
F32 = jnp.float32
BF16 = jnp.bfloat16


def dot(a, b):
    return jnp.dot(a, b, preferred_element_type=F32)


def dot_t(a, b):
    return lax.dot_general(a, b, (((1,), (1,)), ((), ())), preferred_element_type=F32)


def attend(queries, key_rows, values, mask):
    width = queries.shape[-1]
    lane_head = lax.broadcasted_iota(jnp.int32, (1, width), 1) // HEAD_DIM
    total = None
    for head in range(width // HEAD_DIM):
        pick = (lane_head == head).astype(F32).astype(BF16)
        scores = dot_t(queries * pick, key_rows)
        weights = jnp.where(mask, jnp.exp(scores), 0.0)
        probs = weights * (1.0 / jnp.sum(weights, axis=-1, keepdims=True))
        part = dot(probs.astype(BF16), values * pick)
        total = part if total is None else total + part
    return total.astype(BF16)


class Plan:
    def __init__(self, n, n_ta, frames, rows):
        self.n = n
        self.m = frames
        self.unit = rows // frames
        self.low = min(n, frames)
        self.q = frames // self.low
        self.blocks = n_ta * frames // max(n, frames)
        self.u = self.blocks * self.q


def general_kernel(cfg, tok, gain, qkg, wq_h, wo_h, wi_h, wf_h, out, *s):
    n_ta, frames, height, width, plans = cfg
    (stream, gath, wq, wo, wi, wf, pk, a0, a1, res0, res1, att, pk2, att2, pbuf, prec, comb, xrec,
     wsem, ag_s, ag_r, s10, r10, s20, r20, s11, r11, s21, r21, rs_s, rs_r) = s
    rows = tok.shape[0]
    per_frame = height * width
    aw = wo.shape[1]
    me = lax.axis_index("ta")
    core, chip = lax.rem(me, 2), lax.div(me, 2)

    def block_at(k):
        return lax.rem(chip + lax.div(k, 2), 2) * 2 + lax.rem(core + lax.rem(k, 2), 2)

    piece = rows // CHUNKS
    wide = lambda c: pl.ds(pl.multiple_of(c * piece, piece), piece)
    steps = n_ta * CHUNKS
    early = 2 * CHUNKS

    def arrival(i):
        late = i - early
        k = jnp.where(i < early, lax.div(i, CHUNKS), 2 + lax.rem(late, 2))
        c = jnp.where(i < early, lax.rem(i, CHUNKS), lax.div(late, 2))
        return k, c

    def departure(i):
        rest = i - early
        k = jnp.where(i < early, 3 - lax.rem(i, 2), 1 - lax.div(rest, CHUNKS))
        c = jnp.where(i < early, lax.div(i, 2), lax.rem(rest, CHUNKS))
        return k, c

    partner = block_at(1)
    remote = block_at(2)
    pair_last = block_at(3)

    copies = []
    for at in range(3):
        copies.append([
            pltpu.make_async_copy(wq_h.at[at, j], wq.at[at, :, j * aw:(j + 1) * aw], wsem.at[at, j])
            for j in range(3)])
        copies.append([pltpu.make_async_copy(wo_h.at[at], wo.at[at], wsem.at[at, 3])])
    copies.append([pltpu.make_async_copy(wi_h, wi, wsem.at[3, 0])])
    copies.append([pltpu.make_async_copy(wf_h, wf, wsem.at[3, 1])])
    for group in copies:
        for copy in group:
            copy.start()

    def ready(at):
        for copy in copies[at]:
            copy.wait()

    barrier = pltpu.get_barrier_semaphore()
    greets = 0
    for other in (partner, remote):
        pl.semaphore_signal(barrier, inc=1, device_id={"ta": other}, device_id_type=MESH)
        greets += 1
    for axis, plan in plans:
        here = lax.axis_index(axis)
        for step in range(1, plan.n):
            other = lax.rem(here + step, plan.n)
            pl.semaphore_signal(barrier, inc=1, device_id={axis: other}, device_id_type=MESH)
            greets += 1

    def remote_copy(src, dst, send, recv, axis, other):
        return pltpu.make_async_remote_copy(
            src_ref=src, dst_ref=dst, send_sem=send, recv_sem=recv,
            device_id={axis: other}, device_id_type=MESH)

    def norm_own(p, c):
        x = stream[wide(c), :]
        scale = lax.rsqrt(jnp.mean(x * x, axis=-1, keepdims=True) + EPS)
        gath[p, me, wide(c)] = (x * scale * gain[p:p + 1, :]).astype(BF16)

    def ag_copy(p, slot, c):
        block = me if slot < 2 else remote
        other = remote if slot == 1 else partner
        ref = gath.at[p, block, wide(c)]
        return remote_copy(ref, ref, ag_s.at[p, slot, c], ag_r.at[p, slot, c], "ta", other)

    def ag_start(p, c):
        ag_copy(p, 1, c).start()
        ag_copy(p, 0, c).start()

    def ag_wait(p, k, c):
        @pl.when(k == 1)
        def _():
            ag_copy(p, 0, c).wait_recv()

        @pl.when(k == 2)
        def _():
            ag_copy(p, 1, c).wait_recv()
            ag_copy(p, 2, c).start()

        @pl.when(k == 3)
        def _():
            ag_copy(p, 2, c).wait_recv()

    lane_a = lax.broadcasted_iota(jnp.int32, (aw, aw), 0) // HEAD_DIM
    lane_b = lax.broadcasted_iota(jnp.int32, (aw, aw), 1) // HEAD_DIM
    ones = (lane_a == lane_b).astype(F32).astype(BF16)

    def head_norm(x, row):
        square = x * x
        high = square.astype(BF16)
        low = (square - high.astype(F32)).astype(BF16)
        mean = (dot(high, ones) + dot(low, ones)) * (1.0 / HEAD_DIM)
        return x * lax.rsqrt(mean + EPS) * qkg[row:row + 1, :]

    def project(p, b, c):
        flat = dot(gath[p, b, wide(c)], wq[p])
        queries = (head_norm(flat[:, :aw], 2 * p) * (HEAD_DIM ** -0.5)).astype(BF16)
        key_rows = head_norm(flat[:, aw:2 * aw], 2 * p + 1).astype(BF16)
        return queries, key_rows, flat[:, 2 * aw:].astype(BF16)

    def rs_copy(p, slot, c):
        send, recv = rs_s.at[p, slot, c], rs_r.at[p, slot, c]
        if slot == 2:
            return remote_copy(comb.at[p, wide(c)], xrec.at[p, wide(c)], send, recv, "ta", remote)
        return remote_copy(pbuf.at[p, 2 * slot + 1, wide(c)], prec.at[p, slot, wide(c)], send, recv, "ta", partner)

    def rs_put(p, k, c, part):
        pbuf[p, k, wide(c)] = part.astype(BF16)

        @pl.when(k == 1)
        def _():
            rs_copy(p, 0, c).start()

        @pl.when(k == 3)
        def _():
            rs_copy(p, 1, c).start()

    def rs_combine(p, c):
        rs_copy(p, 1, c).wait_recv()
        comb[p, wide(c)] = (pbuf[p, 2, wide(c)].astype(F32) + prec[p, 1, wide(c)].astype(F32)).astype(BF16)
        rs_copy(p, 2, c).start()

    def rs_total(p, c):
        rs_copy(p, 0, c).wait_recv()
        near = pbuf[p, 0, wide(c)].astype(F32) + prec[p, 0, wide(c)].astype(F32)
        rs_copy(p, 2, c).wait_recv()
        return stream[wide(c), :] + (near + xrec[p, wide(c)].astype(F32))

    def turn(p):
        for c in range(CHUNKS):
            stream[wide(c), :] = rs_total(p, c)
            norm_own(p + 1, c)
            ag_start(p + 1, c)

    stream[...] = tok[...].astype(F32)
    norm_own(0, 0)
    pl.semaphore_wait(barrier, greets)
    ag_start(0, 0)
    for c in range(1, CHUNKS):
        norm_own(0, c)
        ag_start(0, c)

    sends = []
    for p in (0, 1):
        axis, plan = plans[p]
        n, m, unit, groups, low, fold, span = plan.n, plan.m, plan.unit, plan.u, plan.low, plan.q, plan.blocks
        here = lax.axis_index(axis)
        abuf, res = ((a0, res0), (a1, res1))[p]
        s1, r1, s2, r2 = ((s10, r10, s20, r20), (s11, r11, s21, r21))[p]
        ready(2 * p)

        def owner_of(b, j, m=m, low=low, span=span):
            return lax.rem(j, low) + m * lax.div(b, span)

        def place(j, unit=unit):
            return pl.ds(pl.multiple_of(j * unit, unit), unit)

        def unit_copy(b, j, p=p, axis=axis, low=low, fold=fold, span=span, here=here, abuf=abuf, s1=s1, r1=r1,
                      owner_of=owner_of, place=place):
            owner = owner_of(b, j)
            u = lax.rem(b, span) * fold + lax.div(j, low)
            return owner, u, remote_copy(
                pk.at[p, b, place(j)], abuf.at[u, here], s1.at[b, j], r1.at[u, here], axis, owner)

        def first(i, _, p=p, m=m, here=here, abuf=abuf, unit_copy=unit_copy, place=place):
            k, c = arrival(i)
            b = block_at(k)
            ag_wait(p, k, c)
            queries, key_rows, values = project(p, b, c)
            pk[p, b, wide(c), 0:aw] = queries
            pk[p, b, wide(c), aw:2 * aw] = key_rows
            pk[p, b, wide(c), 2 * aw:3 * aw] = values
            for at in range(m // CHUNKS):
                j = c * (m // CHUNKS) + at
                owner, u, copy = unit_copy(b, j)

                @pl.when(owner != here)
                def _():
                    copy.start()

                @pl.when(owner == here)
                def _():
                    abuf[u, here] = pk[p, b, place(j), :]
            return 0

        lax.fori_loop(0, steps, first, 0)

        size = n * unit
        if p == 0:
            line_of = lambda at: lax.div(lax.rem(at, unit), width)
        else:
            line_of = lambda at: lax.div(lax.rem(at, unit), per_frame) * width + lax.rem(at, width)
        mask = line_of(lax.broadcasted_iota(jnp.int32, (size, 1), 0)) == line_of(
            lax.broadcasted_iota(jnp.int32, (1, size), 1))

        def home(u, m=m, low=low, fold=fold, span=span, here=here):
            return lax.div(u, fold) + span * lax.div(here, m), lax.rem(here, low) + low * lax.rem(u, fold)

        def back_copy(u, other, p=p, axis=axis, res=res, s2=s2, r2=r2, home=home, place=place):
            b, j = home(u)
            return remote_copy(
                res.at[u, other], att.at[p, b, place(j)], s2.at[u, other], r2.at[b, j], axis, other)

        def second(i, _, p=p, axis=axis, n=n, unit=unit, fold=fold, span=span, here=here, abuf=abuf, res=res,
                   r1=r1, s1=s1, mask=mask, size=size, back_copy=back_copy, home=home, place=place):
            k, sub = arrival(i) if fold == CHUNKS else (lax.div(i, fold), lax.rem(i, fold))
            u = lax.rem(block_at(k), span) * fold + sub
            for step in range(1, n):
                source = lax.rem(here + step, n)
                remote_copy(abuf.at[u, source], abuf.at[u, source], s1.at[0, 0], r1.at[u, source],
                            axis, source).wait_recv()
            done = attend(
                abuf[u, :, :, 0:aw].reshape(size, aw),
                abuf[u, :, :, aw:2 * aw].reshape(size, aw),
                abuf[u, :, :, 2 * aw:3 * aw].reshape(size, aw),
                mask,
            )
            res[u] = done.reshape(n, unit, aw)
            for step in range(1, n):
                back_copy(u, lax.rem(here + step, n)).start()
            b, j = home(u)
            att[p, b, place(j)] = res[u, here]
            return 0

        lax.fori_loop(0, groups, second, 0)
        ready(2 * p + 1)

        def third(i, _, p=p, axis=axis, m=m, here=here, s2=s2, r2=r2, owner_of=owner_of, place=place):
            k, c = departure(i)
            b = block_at(k)
            for at in range(m // CHUNKS):
                j = c * (m // CHUNKS) + at
                owner = owner_of(b, j)

                @pl.when(owner != here)
                def _():
                    ref = att.at[p, b, place(j)]
                    remote_copy(ref, ref, s2.at[0, 0], r2.at[b, j], axis, owner).wait_recv()
            rs_put(p, k, c, dot(att[p, b, wide(c)], wo[p]))

            @pl.when(k == 2)
            def _():
                rs_combine(p, c)
            return 0

        lax.fori_loop(0, steps, third, 0)
        turn(p)

        def drain(unit_copy=unit_copy, back_copy=back_copy, n=n, m=m, groups=groups, here=here):
            for b in range(n_ta):
                for j in range(m):
                    owner, _, copy = unit_copy(b, j)

                    @pl.when(owner != here)
                    def _():
                        copy.wait_send()
            for u in range(groups):
                for step in range(1, n):
                    back_copy(u, lax.rem(here + step, n)).wait_send()

        sends.append(drain)

    p = 2
    some_frames = frames // CHUNKS
    ready(2 * p)

    def time_first(i, _):
        k, c = arrival(i)
        b = block_at(k)
        ag_wait(p, k, c)
        queries, key_rows, values = project(p, b, c)
        at = pl.ds(b * frames + c * some_frames, some_frames)
        pk2[at, :, 0:aw] = queries.reshape(some_frames, per_frame, aw)
        pk2[at, :, aw:2 * aw] = key_rows.reshape(some_frames, per_frame, aw)
        pk2[at, :, 2 * aw:3 * aw] = values.reshape(some_frames, per_frame, aw)
        return 0

    lax.fori_loop(0, steps, time_first, 0)
    every = n_ta * frames
    some = 16
    size = every * some
    i_at = lax.broadcasted_iota(jnp.int32, (size, 1), 0)
    j_at = lax.broadcasted_iota(jnp.int32, (1, size), 1)
    causal = (lax.rem(i_at, some) == lax.rem(j_at, some)) & (lax.div(i_at, some) >= lax.div(j_at, some))

    def time_second(g, _):
        at = pl.ds(pl.multiple_of(g * some, some), some)
        done = attend(
            pk2[:, at, 0:aw].reshape(size, aw),
            pk2[:, at, aw:2 * aw].reshape(size, aw),
            pk2[:, at, 2 * aw:3 * aw].reshape(size, aw),
            causal,
        )
        att2[:, at, :] = done.reshape(every, some, aw)
        return 0

    lax.fori_loop(0, per_frame // some, time_second, 0)
    ready(2 * p + 1)

    def time_third(i, _):
        k, c = departure(i)
        b = block_at(k)
        at = pl.ds(b * frames + c * some_frames, some_frames)
        rs_put(p, k, c, dot(att2[at].reshape(piece, aw), wo[p]))

        @pl.when(k == 2)
        def _():
            rs_combine(p, c)
        return 0

    lax.fori_loop(0, steps, time_third, 0)
    turn(p)

    ready(6)
    ready(7)
    half = wf.shape[0]

    def mlp(i, _):
        k, c = arrival(i)
        b = block_at(k)
        ag_wait(3, k, c)
        both = dot(gath[3, b, wide(c)], wi[...])
        gate, up = both[:, :half], both[:, half:]
        hidden = (gate / (1.0 + jnp.exp(-gate)) * up).astype(BF16)
        rs_put(3, k, c, dot(hidden, wf[...]))

        @pl.when((k == 2) & (c > 0))
        def _():
            rs_combine(3, c - 1)
        return 0

    lax.fori_loop(0, steps, mlp, 0)
    rs_combine(3, CHUNKS - 1)
    for c in range(CHUNKS):
        out[wide(c), :] = rs_total(3, c).astype(BF16)

    for drain in sends:
        drain()
    for p in range(4):
        for slot in range(3):
            for c in range(CHUNKS):
                ag_copy(p, slot, c).wait_send()
                rs_copy(p, slot, c).wait_send()


def general_local(sizes, tokens, norm_gain, qkv_weight, qk_gain, out_weight, ffn_in, ffn_out):
    n_ta, n_ha, n_wa = sizes
    extent = tokens.shape
    clips, frames, height, width, model = extent
    rows = clips * frames * height * width
    aw = qkv_weight.shape[-1]
    half = ffn_in.shape[-1]
    plans = (("wa", Plan(n_wa, n_ta, frames, rows)), ("ha", Plan(n_ha, n_ta, frames, rows)))
    cfg = (n_ta, frames, height, width, plans)
    heads = aw // HEAD_DIM
    gains = jnp.tile(qk_gain.reshape(-1, HEAD_DIM), (1, heads))
    dma = pltpu.SemaphoreType.DMA
    vm = pltpu.VMEM
    scratch = [
        vm((rows, model), F32),
        vm((4, n_ta, rows, model), BF16),
        vm((3, model, 3 * aw), BF16),
        vm((3, aw, model), BF16),
        vm((model, 2 * half), BF16),
        vm((half, model), BF16),
        vm((2, n_ta, rows, 3 * aw), BF16),
    ]
    for width_of in (3 * aw, aw):
        for _, plan in plans:
            scratch.append(vm((plan.u, plan.n, plan.unit, width_of), BF16))
    scratch += [
        vm((2, n_ta, rows, aw), BF16),
        vm((n_ta * frames, height * width, 3 * aw), BF16),
        vm((n_ta * frames, height * width, aw), BF16),
        vm((4, n_ta, rows, model), BF16),
        vm((4, 2, rows, model), BF16),
        vm((4, rows, model), BF16),
        vm((4, rows, model), BF16),
        dma((4, 4)),
        dma((4, 3, CHUNKS)),
        dma((4, 3, CHUNKS)),
    ]
    for _, plan in plans:
        scratch += [
            dma((n_ta, plan.m)),
            dma((plan.u, plan.n)),
            dma((plan.u, plan.n)),
            dma((n_ta, plan.m)),
        ]
    scratch += [dma((4, 3, CHUNKS)), dma((4, 3, CHUNKS))]
    vmem = pl.BlockSpec(memory_space=pltpu.VMEM)
    anyw = pl.BlockSpec(memory_space=pl.ANY)
    result = pl.pallas_call(
        functools.partial(general_kernel, cfg),
        out_shape=jax.ShapeDtypeStruct((rows, model), BF16),
        in_specs=[vmem, vmem, vmem, anyw, anyw, anyw, anyw],
        out_specs=vmem,
        scratch_shapes=scratch,
        compiler_params=pltpu.CompilerParams(
            collective_id=0, has_side_effects=True, vmem_limit_bytes=67043328),
        name="axial_layer",
    )(
        tokens.reshape(rows, model),
        norm_gain,
        gains,
        jnp.transpose(qkv_weight, (0, 2, 1, 3)),
        out_weight,
        ffn_in.reshape(model, 2 * half),
        ffn_out,
    )
    return result.reshape(extent)


def axial_kernel(cfg, tok, gain, qkg, wq_h, wo_h, wi_h, wf_h, out, *s):
    n_ta, n_ha, n_wa, frames, height, width = cfg
    (gains, x0, stream, gath, wq, wo, wi, wf, wi_far, wf_far, sx1, x1, pk2, attb, att, pbuf, prec, fo, ro,
     raw_in, wsem, x0_s, x0_r, ag_s, ag_r, rs_s, rs_r, at_s, at_r, x1_s, x1_r, fo_s, fo_r,
     wx_s, wx_r, wz_s, wz_r, wy_s, wy_r, wd_s, wd_r) = s
    model = tok.shape[-1]
    aw = pk2.shape[-1] // 3
    piece = frames * height * width // CHUNKS
    some_frames = frames // CHUNKS
    sub_rows = height // n_wa
    sub_cols = width // n_ha
    spots = sub_rows * sub_cols
    unit = some_frames * spots
    groups = n_ha * n_wa
    some_groups = groups // CHUNKS
    some_wa = n_wa // CHUNKS
    me = lax.axis_index("ta")
    at_ha = lax.axis_index("ha")
    at_wa = lax.axis_index("wa")
    here = at_wa * n_ha + at_ha
    core, chip = lax.rem(me, 2), lax.div(me, 2)

    def block_at(k):
        return lax.rem(chip + lax.div(k, 2), 2) * 2 + lax.rem(core + lax.rem(k, 2), 2)

    partner = block_at(1)
    remote = block_at(2)
    part_rows = piece // n_wa
    steps = n_ta * CHUNKS
    early = 2 * CHUNKS

    def arrival(i):
        late = i - early
        c = jnp.where(i < early, lax.div(i, 2), lax.div(late, 2))
        k = jnp.where(i < early, lax.rem(i, 2), 2 + lax.rem(late, 2))
        return k, c

    copies = []
    for at in range(3):
        copies.append([
            pltpu.make_async_copy(wq_h.at[at, j], wq.at[at, :, j * aw:(j + 1) * aw], wsem.at[at, j])
            for j in range(3)])
        copies.append([pltpu.make_async_copy(wo_h.at[at], wo.at[at, me], wsem.at[at, 3])])
    copies.append([pltpu.make_async_copy(wi_h, raw_in, wsem.at[3, 0])])
    copies.append([pltpu.make_async_copy(wf_h, wf, wsem.at[3, 1])])

    def ready(at):
        for copy in copies[at]:
            copy.wait()

    barrier = pltpu.get_barrier_semaphore()
    for other in (partner, remote):
        pl.semaphore_signal(barrier, inc=1, device_id={"ta": other}, device_id_type=MESH)

    def group_place(g):
        return {"wa": lax.div(g, n_ha), "ha": lax.rem(g, n_ha)}

    for step in range(1, groups):
        pl.semaphore_signal(barrier, inc=1, device_id=group_place(lax.rem(here + step, groups)), device_id_type=MESH)
    greets = groups + 1

    def remote_copy(src, dst, send, recv, place):
        return pltpu.make_async_remote_copy(
            src_ref=src, dst_ref=dst, send_sem=send, recv_sem=recv,
            device_id=place, device_id_type=MESH)

    for at in (6, 0, 1, 2, 3, 4, 5, 7):
        for copy in copies[at]:
            copy.start()

    def x0_copy(c, source, target):
        at = pl.ds(c * some_frames, some_frames)
        return remote_copy(tok.at[at, target], x0.at[c, source], x0_s.at[c, target], x0_r.at[c, source],
                           {"wa": target})

    flat_rows = model // 16

    def flatten(i, _):
        at = pl.ds(pl.multiple_of(i * flat_rows, flat_rows), flat_rows)
        wi[at] = raw_in[at].reshape(flat_rows, wi.shape[1])
        return 0

    parts_half = wf_h.shape[0] // n_wa
    parts_in = model // wi_far.shape[0]

    def far(j, shard):
        if j < 3:
            return wo.at[j, shard]
        return wi_far.at[j - 3]

    def far_x(j):
        dst = far(j, me).at[at_wa, at_ha]
        if j < 3:
            src = wo_h.at[j, at_wa, at_ha]
        else:
            size = dst.shape[0]
            first = (j - 3) * parts_in
            src = wi.at[pl.ds(pl.multiple_of(first + here * size, size), size)]
        return remote_copy(src, dst, wx_s.at[j], wx_r.at[j], {"ta": remote})

    def half_x(part):
        size = parts_half // n_ha
        src = wf_h.at[pl.ds(pl.multiple_of(at_wa * parts_half + part * size, size), size)]
        return remote_copy(src, wf_far.at[at_wa, part], wz_s.at[5, part], wz_r.at[5, part], {"ta": remote})

    def half_y(part, source, target):
        ref = wf_far.at[source, part]
        return remote_copy(ref, ref, wy_s.at[5, target, part], wy_r.at[5, source, part], {"wa": target})

    def half_start(first, last):
        for part in range(first, last):
            half_x(part).start()

    def half_next(first, last):
        for part in range(first, last):
            half_x(part).wait_recv()
            for step in range(1, n_wa):
                half_y(part, at_wa, lax.rem(at_wa + step, n_wa)).start()

    def half_ready():
        for step in range(1, n_wa):
            source = lax.rem(at_wa + step, n_wa)
            for part in range(n_ha):
                half_y(part, source, source).wait_recv()

    def far_z(j, source, target):
        ref = far(j, remote).at[at_wa, source]
        return remote_copy(ref, ref, wz_s.at[j, target], wz_r.at[j, source], {"ha": target})

    def far_y(j, wa_source, part, target):
        ref = far(j, remote).at[wa_source, part]
        return remote_copy(ref, ref, wy_s.at[j, target, part], wy_r.at[j, wa_source, part], {"wa": target})

    def far_d(j, slot):
        if slot == 0:
            return remote_copy(wo_h.at[j], wo.at[j, me], wd_s.at[j, 0], wd_r.at[j, 0], {"ta": partner})
        ref = wo.at[j, remote]
        return remote_copy(ref, ref, wd_s.at[j, 1], wd_r.at[j, 1], {"ta": partner})

    def far_spread(j, part):
        for step in range(1, n_wa):
            far_y(j, at_wa, part, lax.rem(at_wa + step, n_wa)).start()

    def far_first(j):
        far_x(j).wait_recv()
        for step in range(1, n_ha):
            far_z(j, at_ha, lax.rem(at_ha + step, n_ha)).start()

    def far_own(j):
        far_spread(j, at_ha)

    def far_next(j, first, last):
        for step in range(first, last):
            source = lax.rem(at_ha + step, n_ha)
            far_z(j, source, source).wait_recv()
            far_spread(j, source)

    def far_ready(j):
        for step in range(1, n_wa):
            source = lax.rem(at_wa + step, n_wa)
            for part in range(n_ha):
                far_y(j, source, part, source).wait_recv()

    def far_pair(j):
        far_ready(j)
        far_d(j, 1).start()

    def norm_rows(p, c, at):
        x = stream[p // 2, c, at]
        scale = lax.rsqrt(jnp.mean(x * x, axis=-1, keepdims=True) + EPS)
        gath[p, me, c, at] = (x * scale * gain[p:p + 1, :]).astype(BF16)

    def rows_of(part):
        start = part * part_rows
        return pl.ds(start if isinstance(part, int) else pl.multiple_of(start, part_rows), part_rows)

    def ag_copy(p, slot, c, part):
        block = me if slot < 2 else remote
        other = remote if slot == 1 else partner
        ref = gath.at[p, block, c, rows_of(part)]
        return remote_copy(ref, ref, ag_s.at[p, slot, c, part], ag_r.at[p, slot, c, part], {"ta": other})

    def ag_part(p, c, part):
        ag_copy(p, 1, c, part).start()
        ag_copy(p, 0, c, part).start()

    def norm_start(p, c):
        norm_rows(p, c, pl.ds(0, piece))
        for part in range(n_wa):
            ag_part(p, c, part)

    def ag_wait(p, k, c):
        @pl.when(k == 1)
        def _():
            for part in range(n_wa):
                ag_copy(p, 0, c, part).wait_recv()

        @pl.when(k == 2)
        def _():
            for part in range(n_wa):
                ag_copy(p, 1, c, part).wait_recv()
                ag_copy(p, 2, c, part).start()

        @pl.when(k == 3)
        def _():
            for part in range(n_wa):
                ag_copy(p, 2, c, part).wait_recv()

    lane_a = lax.broadcasted_iota(jnp.int32, (aw, aw), 0) // HEAD_DIM
    lane_b = lax.broadcasted_iota(jnp.int32, (aw, aw), 1) // HEAD_DIM
    ones = (lane_a == lane_b).astype(F32).astype(BF16)

    for p in range(3):
        gains[2 * p:2 * p + 2, :] = jnp.concatenate([qkg[p]] * (aw // HEAD_DIM), axis=1)

    def head_norm(x, row):
        square = x * x
        mean = dot(square.astype(BF16), ones) * (1.0 / HEAD_DIM)
        return x * lax.rsqrt(mean + EPS) * gains[row:row + 1, :]

    def project(p, b, c):
        flat = dot(gath[p, b, c], wq[p])
        queries = (head_norm(flat[:, :aw], 2 * p) * (HEAD_DIM ** -0.5)).astype(BF16)
        key_rows = head_norm(flat[:, aw:2 * aw], 2 * p + 1).astype(BF16)
        return queries, key_rows, flat[:, 2 * aw:].astype(BF16)

    def lanes_of(block):
        return pl.ds(pl.multiple_of(block * aw, aw), aw)

    def att_copy(p, c, source, target):
        return remote_copy(attb.at[p, target, c], att.at[p, c, :, lanes_of(source)],
                           at_s.at[p, c, target], at_r.at[p, c, source], {"ta": target})

    def rs_copy(c):
        return remote_copy(pbuf.at[1, c], prec.at[c], rs_s.at[c], rs_r.at[c], {"ta": partner})

    def total_of(p, c):
        for k in range(1, n_ta):
            source = block_at(k)
            att_copy(p, c, source, source).wait_recv()
        return stream[p // 2, c] + dot(att[p, c], wo[p].reshape(n_ta * aw, model))

    def out_ready(p):
        for slot in range(2):
            far_d(p, slot).wait_recv()

    def pick_rows(source):
        return (source == lax.broadcasted_iota(jnp.int32, (1, piece), 1)).astype(F32).astype(BF16)

    index = lax.broadcasted_iota(jnp.int32, (piece, 1), 0)

    def digits(value, sizes):
        found = []
        for size in sizes[::-1]:
            found.append(lax.rem(value, size))
            value = lax.div(value, size)
        return found[::-1]

    def number(parts, sizes):
        value = parts[0]
        for part, size in zip(parts[1:], sizes[1:]):
            value = value * size + part
        return value

    def x1_copy(c, source, target):
        return remote_copy(sx1.at[c, target], x1.at[c, source], x1_s.at[c, target], x1_r.at[c, source],
                           group_place(target))

    def x1_send(c):
        w, h, f, r, q = digits(index, (n_wa, n_ha, some_frames, sub_rows, sub_cols))
        source = number((w, f, r, h, q), (n_wa, some_frames, sub_rows, n_ha, sub_cols))
        moved = dot(pick_rows(source), total_of(0, c).astype(BF16)).astype(BF16)
        sx1[c] = moved.reshape(groups, unit, model)
        for step in range(1, groups):
            x1_copy(c, here, lax.rem(here + step, groups)).start()
        x1[c, here] = sx1[c, here]

    def x1_take(c):
        for step in range(1, groups):
            source = lax.rem(here + step, groups)
            x1_copy(c, source, source).wait_recv()
        stream[0, c] = x1[c].reshape(piece, model).astype(F32)
        norm_start(1, c)

    def fo_copy(c, source, target):
        return remote_copy(fo.at[c, :, :, target], ro.at[c, source], fo_s.at[c, target], fo_r.at[c, source],
                           {"ha": target})

    def fo_send(c):
        rs_copy(c).wait_recv()
        near = pbuf[0, c].astype(F32) + prec[c].astype(F32)
        total = (stream[1, c] + near).astype(BF16)
        fo[c] = total.reshape(CHUNKS, some_wa, n_ha, unit, model)
        for step in range(1, n_ha):
            fo_copy(c, at_ha, lax.rem(at_ha + step, n_ha)).start()
        ro[c, at_ha] = fo[c, :, :, at_ha]

    def fo_take(c):
        for step in range(1, n_ha):
            source = lax.rem(at_ha + step, n_ha)
            fo_copy(c, source, source).wait_recv()
        f0, f1, w, r, h, q = digits(index, (CHUNKS, some_frames, some_wa, sub_rows, n_ha, sub_cols))
        source = number((h, f0, w, f1, r, q), (n_ha, CHUNKS, some_wa, some_frames, sub_rows, sub_cols))
        moved = dot(pick_rows(source), ro[c].reshape(piece, model)).astype(BF16)
        out[:, c * some_wa:(c + 1) * some_wa] = moved.reshape(frames, some_wa, sub_rows * width, model)

    pl.semaphore_wait(barrier, greets)
    for c in range(CHUNKS):
        for step in range(1, n_wa):
            x0_copy(c, at_wa, lax.rem(at_wa + step, n_wa)).start()
    far_x(0).start()

    def begin(c, part, tokens):
        at = rows_of(part)
        stream[0, c, at] = tokens.reshape(part_rows, model).astype(F32)
        norm_rows(0, c, at)
        ag_part(0, c, part)

    for c in range(CHUNKS):
        begin(c, at_wa, tok[c * some_frames:(c + 1) * some_frames, at_wa])
    for j in range(3):
        far_d(j, 0).start()
    far_x(1).start()
    ready(6)
    lax.fori_loop(0, model // flat_rows, flatten, 0)
    far_first(0)
    for c in range(CHUNKS):
        for step in range(1, n_wa):
            source = lax.rem(at_wa + step, n_wa)
            x0_copy(c, source, source).wait_recv()
            begin(c, source, x0[c, source])
    far_own(0)

    column = lax.broadcasted_iota(jnp.int32, (1, piece), 1)

    def lines_0(at):
        w, f, r, q = digits(at, (n_wa, some_frames, sub_rows, width))
        return f * sub_rows + r

    def lines_1(at):
        g, f, r, q = digits(at, (groups, some_frames, sub_rows, sub_cols))
        return f * sub_cols + q

    def line_step(p, i, mask):
        k, c = arrival(i)
        b = block_at(k)
        ag_wait(p, k, c)
        queries, key_rows, values = project(p, b, c)
        done = attend(queries, key_rows, values, mask)

        @pl.when(k == 0)
        def _():
            att[p, c, :, lanes_of(me)] = done

        @pl.when(k > 0)
        def _():
            attb[p, b, c] = done
            att_copy(p, c, me, b).start()

    def after(i, step, actions):
        @pl.when(i == step)
        def _():
            for action, args in actions:
                action(*args)

    def start_x(j):
        far_x(j).start()

    quarter = n_ha // 2
    ready(0)
    mask_0 = lines_0(index) == lines_0(column)

    def pass_0(i, _):
        line_step(0, i, mask_0)
        after(i, 3, [(far_first, (1,)), (far_own, (1,)), (start_x, (3,))])
        after(i, 4, [(far_next, (0, 1, n_ha))])
        return 0

    lax.fori_loop(0, steps, pass_0, 0)
    for j in (2, 4):
        far_x(j).start()
    half_start(0, quarter)
    far_pair(0)
    ready(1)
    out_ready(0)
    for c in range(CHUNKS):
        x1_send(c)
    far_next(1, 1, n_ha)
    x1_take(0)
    ready(2)
    mask_1 = lines_1(index) == lines_1(column)

    def pass_1(i, _):
        for c in range(1, CHUNKS):
            after(i, 2 * c, [(x1_take, (c,))])
        after(i, 2, [(far_first, (3,)), (far_own, (3,))])
        after(i, 2, [(half_start, (quarter, n_ha)), (half_next, (0, quarter))])
        after(i, 4, [(far_pair, (1,))])
        after(i, 5, [(far_first, (2,)), (far_own, (2,))])
        after(i, 7, [(far_first, (4,)), (far_own, (4,))])
        line_step(1, i, mask_1)
        return 0

    lax.fori_loop(0, steps, pass_1, 0)
    far_next(3, 1, n_ha)
    ready(3)
    out_ready(1)
    half_piece = piece // CHUNKS
    for c in range(CHUNKS):
        total = total_of(1, c)
        for d in range(CHUNKS):
            stream[1, d, c * half_piece:(c + 1) * half_piece] = total[d * half_piece:(d + 1) * half_piece]
    for d in range(CHUNKS):
        norm_start(2, d)
    half_next(quarter, n_ha)
    far_next(2, 1, n_ha)
    for at in (4, 5):
        ready(at)
    t_i = lax.div(index, unit) * some_frames + lax.div(lax.rem(index, unit), spots)
    t_j = lax.div(column, unit) * some_frames + lax.div(lax.rem(column, unit), spots)
    causal = (lax.rem(index, spots) == lax.rem(column, spots)) & (t_i >= t_j)

    def time_project(i, _):
        k, c = arrival(i)
        b = block_at(k)
        ag_wait(2, k, c)
        queries, key_rows, values = project(2, b, c)
        pk2[c, b, :, :, :, 0:aw] = queries.reshape(CHUNKS, some_groups, unit, aw)
        pk2[c, b, :, :, :, aw:2 * aw] = key_rows.reshape(CHUNKS, some_groups, unit, aw)
        pk2[c, b, :, :, :, 2 * aw:3 * aw] = values.reshape(CHUNKS, some_groups, unit, aw)
        return 0

    def time_attend(i, _):
        c = lax.div(i, some_groups)
        g = lax.rem(i, some_groups)
        done = attend(
            pk2[c, :, :, g, :, 0:aw].reshape(piece, aw),
            pk2[c, :, :, g, :, aw:2 * aw].reshape(piece, aw),
            pk2[c, :, :, g, :, 2 * aw:3 * aw].reshape(piece, aw),
            causal,
        )
        for b in range(n_ta):
            for at in range(CHUNKS):
                start = (b * CHUNKS + at) * unit
                rows = pl.ds(pl.multiple_of((at * some_groups + g) * unit, unit), unit)
                attb[2, b, c, rows] = done[start:start + unit]
        return 0

    lax.fori_loop(0, early, time_project, 0)

    def time_chunk(c, _):
        lax.fori_loop(early + 2 * c, early + 2 * c + 2, time_project, 0)

        @pl.when(c == 0)
        def _():
            far_next(4, 1, n_ha)

        lax.fori_loop(c * some_groups, (c + 1) * some_groups, time_attend, 0)
        for k in (2, 3, 1):
            att_copy(2, c, me, block_at(k)).start()
        att[2, c, :, lanes_of(me)] = attb[2, me, c]

        @pl.when(c == 0)
        def _():
            far_pair(2)

        return 0

    lax.fori_loop(0, CHUNKS, time_chunk, 0)

    ready(7)
    out_ready(2)
    half = wf.shape[0]

    def silu_part(x, w_in, w_out):
        both = dot(x, w_in)
        gate, up = both[:, :half], both[:, half:]
        hidden = (gate / (1.0 + jnp.exp(-gate)) * up).astype(BF16)
        return dot(hidden, w_out)

    def mlp(i, _):
        k, c = lax.rem(i, 2), lax.div(i, 2)
        b = block_at(k)

        for d in range(CHUNKS):
            @pl.when(i == 2 * d)
            def _():
                if d > 0:
                    fo_send(d - 1)
                stream[1, d] = total_of(2, d)
                norm_rows(3, d, pl.ds(0, piece))
                for part in range(n_wa):
                    ag_copy(3, 0, d, part).start()

        @pl.when(k == 1)
        def _():
            for part in range(n_wa):
                ag_copy(3, 0, c, part).wait_recv()

        x = gath[3, b, c]
        part = silu_part(x, wi[...], wf[...])

        @pl.when(i == 0)
        def _():
            for j in (3, 4):
                far_ready(j)
            half_ready()

        part += silu_part(x, wi_far[...].reshape(model, 2 * half), wf_far[...].reshape(half, model))
        pbuf[k, c] = part.astype(BF16)

        @pl.when(k == 1)
        def _():
            rs_copy(c).start()

        return 0

    lax.fori_loop(0, 2 * CHUNKS, mlp, 0)
    fo_send(CHUNKS - 1)
    for c in range(CHUNKS):
        fo_take(c)

    for c in range(CHUNKS):
        for step in range(1, n_wa):
            x0_copy(c, at_wa, lax.rem(at_wa + step, n_wa)).wait_send()
        for step in range(1, groups):
            x1_copy(c, here, lax.rem(here + step, groups)).wait_send()
        for step in range(1, n_ha):
            fo_copy(c, at_ha, lax.rem(at_ha + step, n_ha)).wait_send()
        for part in range(n_wa):
            for p in range(3):
                for slot in range(3):
                    ag_copy(p, slot, c, part).wait_send()
            ag_copy(3, 0, c, part).wait_send()
        for p in range(3):
            for k in range(1, n_ta):
                att_copy(p, c, me, block_at(k)).wait_send()
        rs_copy(c).wait_send()
    for part in range(n_ha):
        half_x(part).wait_send()
        for step in range(1, n_wa):
            half_y(part, at_wa, lax.rem(at_wa + step, n_wa)).wait_send()
    for j in range(5):
        far_x(j).wait_send()
        for step in range(1, n_ha):
            far_z(j, at_ha, lax.rem(at_ha + step, n_ha)).wait_send()
        for step in range(1, n_wa):
            for part in range(n_ha):
                far_y(j, at_wa, part, lax.rem(at_wa + step, n_wa)).wait_send()
    for j in range(3):
        for slot in range(2):
            far_d(j, slot).wait_send()


def axial_local(sizes, tokens, norm_gain, qkv_weight, qk_gain, out_weight, ffn_in, ffn_out):
    n_ta, n_ha, n_wa = sizes
    extent = tokens.shape
    clips, frames, height, width, model = extent
    frames = clips * frames
    rows = frames * height * width
    piece = rows // CHUNKS
    aw = qkv_weight.shape[-1]
    half = ffn_in.shape[-1]
    groups = n_ha * n_wa
    unit = piece // groups
    sub = height // n_wa * width
    dma = pltpu.SemaphoreType.DMA
    vm = pltpu.VMEM
    scratch = [
        vm((6, aw), F32),
        vm((CHUNKS, n_wa, frames // CHUNKS, sub, model), BF16),
        vm((2, CHUNKS, piece, model), F32),
        vm((4, n_ta, CHUNKS, piece, model), BF16),
        vm((3, model, 3 * aw), BF16),
        vm((3, n_ta, n_wa, n_ha, aw // groups, model), BF16),
        vm((model, 2 * half), BF16),
        vm((half, model), BF16),
        vm((2, n_wa, n_ha, model // groups // 2, 2 * half), BF16),
        vm((n_wa, n_ha, half // groups, model), BF16),
        vm((CHUNKS, groups, unit, model), BF16),
        vm((CHUNKS, groups, unit, model), BF16),
        vm((CHUNKS, n_ta, CHUNKS, groups // CHUNKS, unit, 3 * aw), BF16),
        vm((3, n_ta, CHUNKS, piece, aw), BF16),
        vm((3, CHUNKS, piece, n_ta * aw), BF16),
        vm((2, CHUNKS, piece, model), BF16),
        vm((CHUNKS, piece, model), BF16),
        vm((CHUNKS, CHUNKS, n_wa // CHUNKS, n_ha, unit, model), BF16),
        vm((CHUNKS, n_ha, CHUNKS, n_wa // CHUNKS, unit, model), BF16),
        vm((model, 2, half), BF16),
        dma((4, 4)),
        dma((CHUNKS, n_wa)),
        dma((CHUNKS, n_wa)),
        dma((4, 3, CHUNKS, n_wa)),
        dma((4, 3, CHUNKS, n_wa)),
        dma((CHUNKS,)),
        dma((CHUNKS,)),
        dma((3, CHUNKS, n_ta)),
        dma((3, CHUNKS, n_ta)),
        dma((CHUNKS, groups)),
        dma((CHUNKS, groups)),
        dma((CHUNKS, n_ha)),
        dma((CHUNKS, n_ha)),
        dma((6,)),
        dma((6,)),
        dma((6, n_ha)),
        dma((6, n_ha)),
        dma((6, n_wa, n_ha)),
        dma((6, n_wa, n_ha)),
        dma((3, 2)),
        dma((3, 2)),
    ]
    vmem = pl.BlockSpec(memory_space=pltpu.VMEM)
    anyw = pl.BlockSpec(memory_space=pl.ANY)
    result = pl.pallas_call(
        functools.partial(axial_kernel, (n_ta, n_ha, n_wa, frames, height, width)),
        out_shape=jax.ShapeDtypeStruct((frames, n_wa, sub, model), BF16),
        in_specs=[vmem, vmem, vmem, anyw, anyw, anyw, anyw],
        out_specs=vmem,
        scratch_shapes=scratch,
        compiler_params=pltpu.CompilerParams(
            collective_id=0, has_side_effects=True, vmem_limit_bytes=67043328),
        name="axial_layer",
    )(
        tokens.reshape(frames, n_wa, sub, model),
        norm_gain,
        qk_gain,
        jnp.transpose(qkv_weight, (0, 2, 1, 3)),
        out_weight.reshape(3, n_wa, n_ha, aw // groups, model),
        ffn_in,
        ffn_out,
    )
    return result.reshape(extent)


def local(sizes, tokens, *weights):
    n_ta, n_ha, n_wa = sizes
    clips, frames, height, width, _ = tokens.shape
    fits = n_wa % CHUNKS == 0 and height % n_wa == 0 and width % n_ha == 0 and clips * frames % CHUNKS == 0
    unit = clips * frames * height * width // (CHUNKS * n_ha * n_wa)
    if fits and unit % 16 == 0:
        return axial_local(sizes, tokens, *weights)
    return general_local(sizes, tokens, *weights)


def solution(mesh):
    sizes = tuple(mesh.shape[name] for name in ("ta", "ha", "wa"))
    return jax.shard_map(
        functools.partial(local, sizes),
        mesh=mesh,
        in_specs=(
            P(None, "ta", "ha", "wa", None),
            P(),
            P(None, None, None, "ta"),
            P(),
            P(None, "ta", None),
            P(None, None, "ta"),
            P("ta", None),
        ),
        out_specs=P(None, "ta", "ha", "wa", None),
        check_vma=False,
    )
```
